32 devices in a mesh: dp: 1 (over z), row: 4 (over y), col: 8 (over x, core).
Axes of the slice: x: 4, y: 4, z: 1, core: 2. Of those that a mesh axis runs over, the one named last changes fastest.
The devices are a block of a 4x4x8 slice.
Arguments:
- pair_rep: bfloat16 [512, 512, 64], P(('dp', 'row'), 'col')
- res_mask: int32 [512], P('dp')
- ln_gamma: float32 [64], replicated
- ln_beta: float32 [64], replicated
- w_q: bfloat16 [64, 64], replicated
- w_k: bfloat16 [64, 64], replicated
- w_v: bfloat16 [64, 64], replicated
- w_b: bfloat16 [64, 4], replicated
- w_g: bfloat16 [64, 64], replicated
- w_o: bfloat16 [64, 64], replicated
Outputs:
- output: bfloat16 [512, 512, 64], P(('dp', 'row'), 'col')
All inputs are finite; a program needn't handle non-finite values.
Results may differ from the reference program's by a relative error of at most 0.00763293.
Values are sent between devices in bfloat16 or wider.
A program may use at most 768 MiB of HBM per device.

```python
import jax
import jax.numpy as jnp
from jax import lax

N = 512
C_Z = 64
HEADS = 4
HEAD = 16
LN_EPS = 1e-5


def layer_norm(pair_rep, ln_gamma, ln_beta):
    pair_f32 = pair_rep.astype(jnp.float32)
    mean_c = jnp.mean(pair_f32, axis=-1, keepdims=True)
    centered = pair_f32 - mean_c
    var_c = jnp.mean(jnp.square(centered), axis=-1, keepdims=True)
    return (centered * lax.rsqrt(var_c + LN_EPS) * ln_gamma + ln_beta).astype(jnp.bfloat16)


def setup_inputs(seed: int = 0, part: int = 0) -> dict:
    part_key = jax.random.fold_in(jax.random.key(seed), part)
    pair_key, len_key = jax.random.split(part_key)
    weight_keys = jax.random.split(jax.random.key(seed + 1), 8)
    proj_dim = HEADS * HEAD
    in_scale = C_Z ** -0.5
    pair_rep = jax.random.normal(pair_key, (N, N, C_Z), jnp.float32).astype(jnp.bfloat16)
    seq_len = jax.random.randint(len_key, (), N // 4, N - N // 8 + 1)
    res_mask = (jnp.arange(N) < seq_len).astype(jnp.int32)
    ln_gamma = 1.0 + 0.5 * jax.random.normal(weight_keys[0], (C_Z,), jnp.float32)
    ln_beta = 0.5 * jax.random.normal(weight_keys[1], (C_Z,), jnp.float32)
    w_q = (jax.random.normal(weight_keys[2], (C_Z, proj_dim), jnp.float32) * in_scale).astype(jnp.bfloat16)
    w_k = (jax.random.normal(weight_keys[3], (C_Z, proj_dim), jnp.float32) * in_scale).astype(jnp.bfloat16)
    w_v = (jax.random.normal(weight_keys[4], (C_Z, proj_dim), jnp.float32) * in_scale).astype(jnp.bfloat16)
    w_b = (jax.random.normal(weight_keys[5], (C_Z, HEADS), jnp.float32) * in_scale).astype(jnp.bfloat16)
    w_g = (jax.random.normal(weight_keys[6], (C_Z, proj_dim), jnp.float32) * in_scale).astype(jnp.bfloat16)
    w_o = (jax.random.normal(weight_keys[7], (proj_dim, C_Z), jnp.float32) * (4.0 * proj_dim ** -0.5)).astype(jnp.bfloat16)
    return {'pair_rep': pair_rep, 'res_mask': res_mask, 'ln_gamma': ln_gamma, 'ln_beta': ln_beta, 'w_q': w_q, 'w_k': w_k, 'w_v': w_v, 'w_b': w_b, 'w_g': w_g, 'w_o': w_o}


def reference(pair_rep, res_mask, ln_gamma, ln_beta, w_q, w_k, w_v, w_b, w_g, w_o):
    proj_dim = HEADS * HEAD
    normed = layer_norm(pair_rep, ln_gamma, ln_beta)
    pair_bias = jnp.dot(normed.reshape(N * N, C_Z), w_b, preferred_element_type=jnp.float32).astype(jnp.bfloat16)
    key_bias = jnp.where(res_mask > 0, 0.0, -1e9).astype(jnp.float32)
    full_bias = pair_bias.reshape(N, N, HEADS).astype(jnp.float32) + key_bias[None, :, None]

    def one_row(row_args):
        pair_row, normed_row = row_args
        queries = (jnp.dot(normed_row, w_q, preferred_element_type=jnp.float32) * HEAD ** -0.5).astype(jnp.bfloat16)
        key_row = jnp.dot(normed_row, w_k, preferred_element_type=jnp.float32).astype(jnp.bfloat16)
        val_row = jnp.dot(normed_row, w_v, preferred_element_type=jnp.float32).astype(jnp.bfloat16)
        gate_vals = jax.nn.sigmoid(jnp.dot(normed_row, w_g, preferred_element_type=jnp.float32))
        logits = jnp.einsum('jhd,khd->jkh', queries.reshape(N, HEADS, HEAD).astype(jnp.float32), key_row.reshape(N, HEADS, HEAD).astype(jnp.float32)) + full_bias
        weights = jax.nn.softmax(logits, axis=1)
        attended = jnp.einsum('jkh,khd->jhd', weights, val_row.reshape(N, HEADS, HEAD).astype(jnp.float32))
        gated_out = (gate_vals * attended.reshape(N, proj_dim)).astype(jnp.bfloat16)
        update = jnp.dot(gated_out, w_o, preferred_element_type=jnp.float32)
        return (pair_row.astype(jnp.float32) + update).astype(jnp.bfloat16)

    return lax.map(one_row, (pair_rep, normed))
```

```python
import functools

import jax
import jax.numpy as jnp
from jax import lax
from jax.experimental import pallas as pl
from jax.experimental.pallas import tpu as pltpu
from jax.sharding import PartitionSpec as P

LN_EPS = 1e-5
F32 = jnp.float32
BF16 = jnp.bfloat16
MESH = pl.DeviceIdType.MESH


def pack_kernel(z_ref, wb_ref, gamma_ref, beta_ref, zt_ref, bias_ref, acc_ref):
    group = pl.program_id(0)
    rows, cols, chan = z_ref.shape
    half = rows // 2
    heads = bias_ref.shape[0]
    normed = []
    for t in range(half):
        pair = jnp.concatenate([z_ref[t], z_ref[t + half]], axis=0).astype(F32)
        zt = pair.T
        zt_ref[0, t] = zt.astype(BF16)
        mean = jnp.mean(zt, axis=0, keepdims=True)
        cen = zt - mean
        var = jnp.mean(cen * cen, axis=0, keepdims=True)
        normed.append((cen * lax.rsqrt(var + LN_EPS) * gamma_ref[...] + beta_ref[...]).astype(BF16))
    stacked = jnp.concatenate(normed, axis=0)
    bias = jnp.dot(wb_ref[...], stacked, preferred_element_type=F32)
    for h in range(heads):
        acc_ref[h, pl.ds(pl.multiple_of(group * half, half), half), :] = bias[h * half:(h + 1) * half]

    @pl.when(group == pl.num_programs(0) - 1)
    def _():
        n_q = acc_ref.shape[1]
        src = lax.broadcasted_iota(jnp.int32, (n_q, 2 * n_q), 0)
        dst = lax.broadcasted_iota(jnp.int32, (n_q, 2 * n_q), 1)
        base = (src // half) * rows + src % half
        sel0 = jnp.where(dst == base, 1.0, 0.0).astype(BF16)
        sel1 = jnp.where(dst == base + half, 1.0, 0.0).astype(BF16)
        for h in range(heads):
            tr = acc_ref[h].T.astype(BF16)
            out = jnp.dot(tr[:cols], sel0, preferred_element_type=F32)
            out = out + jnp.dot(tr[cols:], sel1, preferred_element_type=F32)
            bias_ref[h] = out.astype(BF16)


def unpack_kernel(r_ref, out_ref):
    half = r_ref.shape[1]
    cols = out_ref.shape[1]
    for t in range(half):
        pair = r_ref[0, t].astype(F32).T.astype(BF16)
        out_ref[t] = pair[:cols]
        out_ref[t + half] = pair[cols:]


def project(t, zbuf, w_t, gamma, beta, heads, zr, qz, kr, vr, gr):
    n_src, _, chan, lanes = zbuf.shape
    half = lanes // 2
    n = n_src * half
    hd = chan // heads
    low = lax.broadcasted_iota(jnp.int32, (chan, lanes), 1) < half
    blk = [zbuf[c, t].astype(F32) for c in range(n_src)]
    rows = ([], [])
    for x in range(n_src // 2):
        a, b = blk[2 * x], blk[2 * x + 1]
        rows[0].append(jnp.where(low, a, pltpu.roll(b, half, 1)))
        rows[1].append(jnp.where(low, pltpu.roll(a, half, 1), b))
    for side in range(2):
        r = 2 * t + side
        z = jnp.concatenate(rows[side], axis=1)
        zr[r] = z
        mean = jnp.mean(z, axis=0, keepdims=True)
        cen = z - mean
        var = jnp.mean(cen * cen, axis=0, keepdims=True)
        normed = (cen * lax.rsqrt(var + LN_EPS) * gamma + beta).astype(BF16)
        proj = jnp.dot(w_t, normed, preferred_element_type=F32)
        q_t = (proj[:chan] * hd ** -0.5).astype(BF16)
        for h in range(heads):
            parts = []
            if h > 0:
                parts.append(jnp.zeros((h * hd, n), BF16))
            parts.append(q_t[h * hd:(h + 1) * hd])
            if h < heads - 1:
                parts.append(jnp.zeros(((heads - 1 - h) * hd, n), BF16))
            qz[r * heads + h] = jnp.concatenate(parts, axis=0)
            vr[r * heads + h] = proj[2 * chan + h * hd:2 * chan + (h + 1) * hd].astype(BF16)
            gr[r * heads + h] = jax.nn.sigmoid(proj[3 * chan + h * hd:3 * chan + (h + 1) * hd])
        kr[r] = proj[chan:2 * chan].T.astype(BF16)


KC = 64
TK = 256
TN = 256


def unit(u, n_unit, heads, bias, qz, kr, vr, gr, sref, mref, gat, do_ex=True, do_qk=True):
    n = sref.shape[-1]
    if do_qk:
        nxt = u + 1 if isinstance(u, int) else jnp.minimum(u + 1, n_unit - 1)
        s = jnp.dot(kr[nxt // heads], qz[nxt], preferred_element_type=F32)
    if do_ex:
        v = vr[u]
        g = gr[u]
        outs = []
        for nb in range(n // TN):
            ns = slice(nb * TN, (nb + 1) * TN)
            mb = jnp.broadcast_to(mref[:, ns], (8, TN))
            total = jnp.zeros((8, TN), F32)
            o = None
            for tk in range(n // TK):
                ks = slice(tk * TK, (tk + 1) * TK)
                p = jnp.exp(sref[ks, ns].reshape(TK // 8, 8, TN) - mb[None])
                total = total + jnp.sum(p, axis=0)
                d = jnp.dot(v[:, ks], p.reshape(TK, TN).astype(BF16), preferred_element_type=F32)
                o = d if o is None else o + d
            outs.append((g[:, ns] * (o / jnp.sum(total, axis=0, keepdims=True))).astype(BF16))
        gat[u] = jnp.concatenate(outs, axis=1)
    if do_qk:
        h = nxt % heads
        top = None
        for kc in range(n // KC):
            sl = slice(kc * KC, (kc + 1) * KC)
            sc = s[sl] + bias[h, sl, :]
            sref[sl, :] = sc
            m8 = jnp.max(sc.reshape(KC // 8, 8, n), axis=0)
            top = m8 if top is None else jnp.maximum(top, m8)
        mref[...] = jnp.max(top, axis=0, keepdims=True)


def finish(t, zr, gat, wo_t, heads, obuf):
    n_src, _, chan, lanes = obuf.shape
    half = lanes // 2
    low = lax.broadcasted_iota(jnp.int32, (chan, lanes), 1) < half
    o = []
    for side in range(2):
        r = 2 * t + side
        gated = jnp.concatenate([gat[r * heads + h] for h in range(heads)], axis=0)
        o.append(zr[r] + jnp.dot(wo_t, gated, preferred_element_type=F32))
    for x in range(n_src // 2):
        a = o[0][:, x * lanes:(x + 1) * lanes]
        b = o[1][:, x * lanes:(x + 1) * lanes]
        obuf[2 * x, t] = jnp.where(low, a, pltpu.roll(b, half, 1)).astype(BF16)
        obuf[2 * x + 1, t] = jnp.where(low, pltpu.roll(a, half, 1), b).astype(BF16)


def attn_kernel(n_col, n_row, zt, bt, kb, w_t, wo_t, gamma, beta, res,
                zbuf, ball, bias, zr, qz, kr, vr, gr, sref, mref, gat, obuf,
                b1_send, b1_recv, z_send, z_recv, b2_send, b2_recv, b3_send, b3_recv,
                o_send, o_recv, own_sem):
    col = lax.axis_index('col')
    row = lax.axis_index('row')
    core = lax.rem(col, 2)
    mate = col + 1 - 2 * core
    heads = bt.shape[0]
    hh = heads // 2
    n_pair = zbuf.shape[1]
    cols = bt.shape[1]

    def at_col(d):
        return lax.rem(col + d, n_col)

    def at_row(d):
        return lax.rem(row + d, n_row)

    barrier = pltpu.get_barrier_semaphore()
    for d in range(1, n_col):
        pl.semaphore_signal(barrier, inc=1, device_id={'col': at_col(d)}, device_id_type=MESH)
    for d in range(1, n_row):
        pl.semaphore_signal(barrier, inc=1, device_id={'row': at_row(d)}, device_id_type=MESH)
    pl.semaphore_wait(barrier, n_col + n_row - 2)

    key_rows = pl.ds(pl.multiple_of(col * cols, cols), cols)
    my_heads = pl.ds(core * hh, hh)

    b1 = []
    for d in range(1, n_col):
        peer = at_col(d)
        side = lax.rem(peer, 2)
        b1.append(pltpu.make_async_remote_copy(
            src_ref=bt.at[pl.ds(side * hh, hh)],
            dst_ref=ball.at[row, pl.ds(side * hh, hh), key_rows, :],
            send_sem=b1_send.at[d - 1], recv_sem=b1_recv.at[d - 1],
            device_id={'col': peer}, device_id_type=MESH))
        b1[-1].start()
    zc = []
    for d in range(1, n_col):
        peer = at_col(d)
        zc.append(pltpu.make_async_remote_copy(
            src_ref=zt.at[peer], dst_ref=zbuf.at[col],
            send_sem=z_send.at[d - 1], recv_sem=z_recv.at[d - 1],
            device_id={'col': peer}, device_id_type=MESH))
        zc[-1].start()
    zbuf[col] = zt[col]
    ball[row, my_heads, key_rows, :] = bt[my_heads]

    for c in b1:
        c.wait_recv()
    b2 = []
    for d in range(1, n_row):
        b2.append(pltpu.make_async_remote_copy(
            src_ref=ball.at[row, my_heads], dst_ref=ball.at[row, my_heads],
            send_sem=b2_send.at[d - 1], recv_sem=b2_recv.at[d - 1],
            device_id={'row': at_row(d)}, device_id_type=MESH))
        b2[-1].start()
    b3 = []
    b3.append(pltpu.make_async_remote_copy(
        src_ref=ball.at[row, my_heads], dst_ref=ball.at[row, my_heads],
        send_sem=b3_send.at[0], recv_sem=b3_recv.at[0],
        device_id={'col': mate}, device_id_type=MESH))
    b3[-1].start()

    for c in zc:
        c.wait_recv()
    w = w_t[...]
    ga = gamma[...]
    be = beta[...]

    def project_body(t, carry):
        project(t, zbuf, w, ga, be, heads, zr, qz, kr, vr, gr)
        return carry

    lax.fori_loop(0, n_pair, project_body, 0)

    for d in range(1, n_row):
        b2[d - 1].wait_recv()
        src_row = lax.rem(row + n_row - d, n_row)
        b3.append(pltpu.make_async_remote_copy(
            src_ref=ball.at[src_row, my_heads], dst_ref=ball.at[src_row, my_heads],
            send_sem=b3_send.at[d], recv_sem=b3_recv.at[d],
            device_id={'col': mate}, device_id_type=MESH))
        b3[-1].start()
    for c in b3:
        c.wait_recv()

    strip = ball.shape[-1]
    for r in range(n_row):
        for h in range(heads):
            bias[h, :, r * strip:(r + 1) * strip] = ball[r, h].astype(F32) + kb[...]

    n_unit = n_pair * 2 * heads
    step = functools.partial(unit, n_unit=n_unit, heads=heads, bias=bias, qz=qz, kr=kr, vr=vr,
                             gr=gr, sref=sref, mref=mref, gat=gat)
    wo = wo_t[...]

    def out_copy(d, t):
        peer = at_col(d)
        return pltpu.make_async_remote_copy(
            src_ref=obuf.at[peer, t], dst_ref=res.at[col, t],
            send_sem=o_send.at[d - 1], recv_sem=o_recv.at[d - 1],
            device_id={'col': peer}, device_id_type=MESH)

    step(-1, do_ex=False)

    def pair_body(t, carry):
        def unit_body(i, c):
            step(t * 2 * heads + i)
            return c
        lax.fori_loop(0, 2 * heads, unit_body, 0)
        finish(t, zr, gat, wo, heads, obuf)
        for d in range(1, n_col):
            out_copy(d, t).start()
        return carry

    lax.fori_loop(0, n_pair, pair_body, 0)

    own = pltpu.make_async_copy(obuf.at[col], res.at[col], own_sem)
    own.start()
    for c in b1 + zc + b2 + b3:
        c.wait_send()
    for d in range(1, n_col):
        peer = at_col(d)
        whole = pltpu.make_async_remote_copy(
            src_ref=obuf.at[peer], dst_ref=res.at[col],
            send_sem=o_send.at[d - 1], recv_sem=o_recv.at[d - 1],
            device_id={'col': peer}, device_id_type=MESH)
        whole.wait_send()
        whole.wait_recv()
    own.wait()


def solution(mesh):
    n_col = mesh.shape['col']
    n_row = mesh.shape['row']
    tile_spec = P(('dp', 'row'), 'col', None)
    vmem = pl.BlockSpec(memory_space=pltpu.VMEM)

    def per_device(pair_tile, res_mask, ln_gamma, ln_beta, w_q, w_k, w_v, w_b, w_g, w_o):
        row_len, col_len, chan = pair_tile.shape
        heads = w_b.shape[1]
        hd = chan // heads
        n = res_mask.shape[0]
        own = row_len // n_col
        half = own // 2
        gamma = ln_gamma.reshape(chan, 1)
        beta = ln_beta.reshape(chan, 1)
        eye = jnp.eye(half, dtype=w_b.dtype)
        wb_big = (w_b.T[:, None, None, :] * eye[None, :, :, None]).reshape(heads * half, half * chan)
        w_t = jnp.concatenate([w_q, w_k, w_v, w_g], axis=1).T
        wo_t = w_o.T
        kb = jnp.broadcast_to(jnp.where(res_mask > 0, 0.0, -1e9).astype(F32)[:, None], (n, row_len))

        zt, bt = pl.pallas_call(
            pack_kernel,
            grid=(n_col,),
            in_specs=[pl.BlockSpec((own, col_len, chan), lambda i: (i, 0, 0)), vmem, vmem, vmem],
            out_specs=[pl.BlockSpec((1, half, chan, 2 * col_len), lambda i: (i, 0, 0, 0)),
                       pl.BlockSpec((heads, col_len, row_len), lambda i: (0, 0, 0))],
            out_shape=[jax.ShapeDtypeStruct((n_col, half, chan, 2 * col_len), BF16),
                       jax.ShapeDtypeStruct((heads, col_len, row_len), BF16)],
            scratch_shapes=[pltpu.VMEM((heads, row_len // 2, 2 * col_len), F32)],
            name='pack',
        )(pair_tile, wb_big, gamma, beta)

        dma = pltpu.SemaphoreType.DMA
        res = pl.pallas_call(
            functools.partial(attn_kernel, n_col, n_row),
            in_specs=[vmem] * 7,
            out_specs=pl.BlockSpec(memory_space=pl.ANY),
            out_shape=jax.ShapeDtypeStruct((n_col, half, chan, 2 * col_len), BF16),
            scratch_shapes=[
                pltpu.VMEM((n_col, half, chan, 2 * col_len), BF16),
                pltpu.VMEM((n_row, heads, n, row_len), BF16),
                pltpu.VMEM((heads, n, n), F32),
                pltpu.VMEM((own, chan, n), F32),
                pltpu.VMEM((own * heads, chan, n), BF16),
                pltpu.VMEM((own, n, chan), BF16),
                pltpu.VMEM((own * heads, hd, n), BF16),
                pltpu.VMEM((own * heads, hd, n), F32),
                pltpu.VMEM((n, n), F32),
                pltpu.VMEM((1, n), F32),
                pltpu.VMEM((own * heads, hd, n), BF16),
                pltpu.VMEM((n_col, half, chan, 2 * col_len), BF16),
                dma((n_col - 1,)), dma((n_col - 1,)), dma((n_col - 1,)), dma((n_col - 1,)),
                dma((n_row - 1,)), dma((n_row - 1,)), dma((n_row,)), dma((n_row,)),
                dma((n_col - 1,)), dma((n_col - 1,)), dma,
            ],
            compiler_params=pltpu.CompilerParams(
                collective_id=0, has_side_effects=True, vmem_limit_bytes=48 << 20),
            name='attention',
        )(zt, bt, kb, w_t, wo_t, gamma, beta)

        return pl.pallas_call(
            unpack_kernel,
            grid=(n_col,),
            in_specs=[pl.BlockSpec((1, half, chan, 2 * col_len), lambda i: (i, 0, 0, 0))],
            out_specs=pl.BlockSpec((own, col_len, chan), lambda i: (i, 0, 0)),
            out_shape=jax.ShapeDtypeStruct((row_len, col_len, chan), BF16),
            name='unpack',
        )(res)

    return jax.shard_map(per_device, mesh=mesh,
                         in_specs=(tile_spec, P('dp'), P(), P(), P(), P(), P(), P(), P(), P()),
                         out_specs=tile_spec, check_vma=False)
```

```python
import functools

import jax
import jax.numpy as jnp
from jax import lax
from jax.experimental import pallas as pl
from jax.experimental.pallas import tpu as pltpu
from jax.sharding import PartitionSpec as P

LN_EPS = 1e-5
F32 = jnp.float32
BF16 = jnp.bfloat16
MESH = pl.DeviceIdType.MESH

ROWS = 2
KEYS = 64
TILE = 256


def column(row, lanes):
    return jnp.broadcast_to(row, (lanes, row.shape[-1])).T


def layer_norm(z, gamma, beta, axis):
    mean = jnp.mean(z, axis=axis, keepdims=True)
    cen = z - mean
    var = jnp.mean(cen * cen, axis=axis, keepdims=True)
    return (cen * lax.rsqrt(var + LN_EPS) * gamma + beta).astype(BF16)


def tile_bias(zin, wb_t, gamma, beta, bt):
    n_key, chan, n_q = zin.shape
    heads = bt.shape[0]
    group = 16
    wide = jnp.concatenate([wb_t, wb_t], axis=1)
    wide = jnp.concatenate([wide] * (group // 2), axis=1)
    rows = jnp.concatenate([jnp.broadcast_to(wide[h:h + 1], (group, group * chan)) for h in range(heads)], axis=0)
    own = lax.broadcasted_iota(jnp.int32, rows.shape, 0) % group
    src = lax.broadcasted_iota(jnp.int32, rows.shape, 1) // chan
    big = jnp.where(own == src, rows, 0.0).astype(BF16)

    def body(g, carry):
        start = pl.multiple_of(g * group, group)
        normed = layer_norm(zin[pl.ds(start, group)].astype(F32), gamma[None], beta[None], 1)
        out = jnp.dot(big, normed.reshape(group * chan, n_q), preferred_element_type=F32)
        for h in range(heads):
            bt[h, pl.ds(start, group), :] = out[h * group:(h + 1) * group].astype(BF16)
        return carry

    lax.fori_loop(0, n_key // group, body, 0)


def to_rows(zin, zt):
    n_key, chan, _ = zin.shape
    hc = chan // 2
    for s in range(0, hc, 16):
        a = jnp.swapaxes(zin[:, s:s + 16, :].astype(F32), 0, 1)
        b = jnp.swapaxes(zin[:, hc + s:hc + s + 16, :].astype(F32), 0, 1)
        c = jnp.concatenate([a, b], axis=1)
        c = jnp.stack([c[i].T for i in range(16)], axis=0)
        zt[:, s:s + 16, :] = jnp.swapaxes(c, 0, 1).astype(BF16)


def unpack_kernel(r, out):
    n_key, chan, _ = out.shape
    hc = chan // 2
    for s in range(0, hc, 16):
        c = jnp.swapaxes(r[:, s:s + 16, :].astype(F32), 0, 1)
        c = [c[i].T for i in range(16)]
        a = jnp.stack([x[:n_key] for x in c], axis=0)
        b = jnp.stack([x[n_key:] for x in c], axis=0)
        out[:, s:s + 16, :] = jnp.swapaxes(a, 0, 1).astype(BF16)
        out[:, hc + s:hc + s + 16, :] = jnp.swapaxes(b, 0, 1).astype(BF16)


def project(t, zbuf, w_t, gamma, beta, heads, zr, qz, kr, vr, gr):
    n_src, _, hc, lanes = zbuf.shape
    chan = 2 * hc
    half = lanes // 2
    n = n_src * half
    hd = chan // heads
    low = lax.broadcasted_iota(jnp.int32, (hc, lanes), 1) < half
    for side in range(ROWS):
        r = ROWS * t + side
        cols = []
        for x in range(n_src // 2):
            a = zbuf[2 * x, r].astype(F32)
            b = zbuf[2 * x + 1, r].astype(F32)
            top = jnp.where(low, a, pltpu.roll(b, half, 1))
            bot = jnp.where(low, pltpu.roll(a, half, 1), b)
            cols.append(jnp.concatenate([top, bot], axis=0))
        z = jnp.concatenate(cols, axis=1)
        zr[r] = z
        proj = jnp.dot(w_t, layer_norm(z, gamma, beta, 0), preferred_element_type=F32)
        q_t = (proj[:chan] * hd ** -0.5).astype(BF16)
        for h in range(heads):
            parts = []
            if h > 0:
                parts.append(jnp.zeros((h * hd, n), BF16))
            parts.append(q_t[h * hd:(h + 1) * hd])
            if h < heads - 1:
                parts.append(jnp.zeros(((heads - 1 - h) * hd, n), BF16))
            qz[r * heads + h] = jnp.concatenate(parts, axis=0)
            vr[r * heads + h] = proj[2 * chan + h * hd:2 * chan + (h + 1) * hd].astype(BF16)
            gr[r * heads + h] = jax.nn.sigmoid(proj[3 * chan + h * hd:3 * chan + (h + 1) * hd])
        kr[r] = proj[chan:2 * chan].T.astype(BF16)


class Logits:
    def __init__(self, slot, row, head, heads, bias, qz, kr, sref, mref):
        self.slot, self.head, self.bias, self.sref, self.mref = slot, head, bias, sref, mref
        self.value = jnp.dot(kr[row], qz[row * heads + head], preferred_element_type=F32)
        self.top = None
        self.done = 0

    def advance(self):
        n = self.sref.shape[-1]
        if self.done == n:
            return
        sl = slice(self.done, self.done + KEYS)
        self.done += KEYS
        part = self.value[sl] + self.bias[self.head, sl, :]
        self.sref[self.slot, sl, :] = part
        top = jnp.max(part.reshape(KEYS // 8, 8, n), axis=0)
        self.top = top if self.top is None else jnp.maximum(self.top, top)

    def end(self):
        while self.done < self.sref.shape[-1]:
            self.advance()
        self.mref[self.slot] = jnp.max(self.top, axis=0, keepdims=True)


def step(s, n_pair, heads, bias, qz, kr, vr, gr, sref, mref, gat, do_ex=True):
    n = sref.shape[-1]
    hh = heads // 2
    nxt = s + 1 if isinstance(s, int) else jnp.minimum(s + 1, n_pair * hh - 1)

    def place(at, i):
        return (at % n_pair) * ROWS + i // 2, at // n_pair + hh * (i % 2)

    pending = None
    for i in range(2 * ROWS):
        row, head = place(nxt, i)
        logits = Logits(i, row, head, heads, bias, qz, kr, sref, mref)
        if do_ex:
            row, head = place(s, i)
            idx = row * heads + head
            v = vr[idx]
            g = gr[idx]
            outs = []
            for q0 in range(0, n, TILE):
                qs = slice(q0, q0 + TILE)
                peak = jnp.broadcast_to(mref[i, :, qs], (8, TILE))[None]
                total = jnp.zeros((8, TILE), F32)
                acc = None
                for k0 in range(0, n, TILE):
                    parts = []
                    for k1 in range(k0, k0 + TILE, KEYS):
                        p = jnp.exp(sref[i, k1:k1 + KEYS, qs].reshape(KEYS // 8, 8, TILE) - peak)
                        total = total + jnp.sum(p, axis=0)
                        parts.append(p.reshape(KEYS, TILE).astype(BF16))
                        if pending is not None:
                            pending.advance()
                    d = jnp.dot(v[:, k0:k0 + TILE], jnp.concatenate(parts, axis=0), preferred_element_type=F32)
                    acc = d if acc is None else acc + d
                outs.append((g[:, qs] * (acc / jnp.sum(total, axis=0, keepdims=True))).astype(BF16))
            gat[idx] = jnp.concatenate(outs, axis=1)
        if pending is not None:
            pending.end()
        pending = logits
    pending.end()


def finish(t, zr, gat, wo_t, heads, obuf):
    n_src, _, hc, lanes = obuf.shape
    half = lanes // 2
    low = lax.broadcasted_iota(jnp.int32, (hc, lanes), 1) < half
    for side in range(ROWS):
        r = ROWS * t + side
        gated = jnp.concatenate([gat[r * heads + h] for h in range(heads)], axis=0)
        o = zr[r] + jnp.dot(wo_t, gated, preferred_element_type=F32)
        for x in range(n_src // 2):
            top = o[:hc, x * lanes:(x + 1) * lanes]
            bot = o[hc:, x * lanes:(x + 1) * lanes]
            obuf[2 * x, r] = jnp.where(low, top, pltpu.roll(bot, half, 1)).astype(BF16)
            obuf[2 * x + 1, r] = jnp.where(low, pltpu.roll(top, half, 1), bot).astype(BF16)


def attn_kernel(n_col, n_row, zin, mask, gamma_row, beta_row, w_q, w_k, w_v, w_g, wb_t, w_o, res,
                bt, zt, zbuf, ball, bias, kb, zr, qz, kr, vr, gr, sref, mref, gat, obuf,
                b1_send, b1_recv, z_send, z_recv, b2_send, b2_recv, b3_send, b3_recv,
                o_send, o_recv, own_sem):
    col = lax.axis_index('col')
    row = lax.axis_index('row')
    core = lax.rem(col, 2)
    mate = col + 1 - 2 * core
    heads, cols, strip = bt.shape
    hh = heads // 2
    own = zbuf.shape[1]
    n_pair = own // ROWS
    n = sref.shape[-1]

    def at_col(d):
        return lax.rem(col + d, n_col)

    def at_row(d):
        return lax.rem(row + d, n_row)

    def remote(src, dst, send, recv, where):
        return pltpu.make_async_remote_copy(src_ref=src, dst_ref=dst, send_sem=send, recv_sem=recv,
                                            device_id=where, device_id_type=MESH)

    barrier = pltpu.get_barrier_semaphore()
    for d in range(1, n_col):
        pl.semaphore_signal(barrier, inc=1, device_id={'col': at_col(d)}, device_id_type=MESH)
    for d in range(1, n_row):
        pl.semaphore_signal(barrier, inc=1, device_id={'row': at_row(d)}, device_id_type=MESH)

    ga = column(gamma_row[...], strip)
    be = column(beta_row[...], strip)
    tile_bias(zin, wb_t[...].astype(F32), ga, be, bt)
    pl.semaphore_wait(barrier, n_col + n_row - 2)

    key_rows = pl.ds(pl.multiple_of(col * cols, cols), cols)
    my_heads = pl.ds(core * hh, hh)
    b1 = []
    for d in range(1, n_col):
        peer = at_col(d)
        half = pl.ds(lax.rem(peer, 2) * hh, hh)
        b1.append(remote(bt.at[half], ball.at[row, half, key_rows, :],
                         b1_send.at[d - 1], b1_recv.at[d - 1], {'col': peer}))
        b1[-1].start()
    ball[row, my_heads, key_rows, :] = bt[my_heads]

    to_rows(zin, zt)
    part = own // 2
    zc = [[], []]
    for e in range(2):
        for d in range(1, n_col):
            peer = at_col(d)
            zc[e].append(remote(zt.at[pl.ds(peer * own + e * part, part)],
                                zbuf.at[col, pl.ds(e * part, part)],
                                z_send.at[e, d - 1], z_recv.at[e, d - 1], {'col': peer}))
            zc[e][-1].start()
    zbuf[col] = zt[pl.ds(col * own, own)]

    for c in b1:
        c.wait_recv()
    b2 = [[], []]
    b3 = [[], []]
    for e in range(hh):
        head = core * hh + e
        for d in range(1, n_row):
            b2[e].append(remote(ball.at[row, head], ball.at[row, head],
                                b2_send.at[e, d - 1], b2_recv.at[e, d - 1], {'row': at_row(d)}))
            b2[e][-1].start()
        b3[e].append(remote(ball.at[row, head], ball.at[row, head],
                            b3_send.at[e, 0], b3_recv.at[e, 0], {'col': mate}))
        b3[e][-1].start()

    def pass_on(e):
        head = core * hh + e
        for d in range(1, n_row):
            b2[e][d - 1].wait_recv()
            from_row = lax.rem(row + n_row - d, n_row)
            b3[e].append(remote(ball.at[from_row, head], ball.at[from_row, head],
                                b3_send.at[e, d], b3_recv.at[e, d], {'col': mate}))
            b3[e][-1].start()

    def take_bias(e):
        for c in b3[e]:
            c.wait_recv()
        for h in range(e, heads, hh):
            for r in range(n_row):
                bias[h, :, r * strip:(r + 1) * strip] = ball[r, h].astype(F32) + kb[...]

    kb[...] = column(jnp.where(mask[...] > 0, 0.0, -1e9).astype(F32), strip)
    w_t = jnp.concatenate([w[...].astype(F32).T for w in (w_q, w_k, w_v, w_g)], axis=0).astype(BF16)
    wo_t = w_o[...].astype(F32).T.astype(BF16)
    ga_n = jnp.concatenate([ga] * (n // strip), axis=1)
    be_n = jnp.concatenate([be] * (n // strip), axis=1)

    def project_body(t, carry):
        project(t, zbuf, w_t, ga_n, be_n, heads, zr, qz, kr, vr, gr)
        return carry

    for c in zc[0]:
        c.wait_recv()
    lax.fori_loop(0, n_pair // 2, project_body, 0)
    pass_on(0)
    for c in zc[1]:
        c.wait_recv()
    lax.fori_loop(n_pair // 2, n_pair, project_body, 0)
    take_bias(0)

    run = functools.partial(step, n_pair=n_pair, heads=heads, bias=bias, qz=qz, kr=kr, vr=vr,
                            gr=gr, sref=sref, mref=mref, gat=gat)

    def early_body(s, carry):
        run(s)
        return carry

    run(-1, do_ex=False)
    lax.fori_loop(0, n_pair // 2, early_body, 0)
    pass_on(1)
    lax.fori_loop(n_pair // 2, n_pair - 1, early_body, 0)
    take_bias(1)
    run(n_pair - 1)

    def late_body(t, carry):
        run(n_pair + t)
        finish(t, zr, gat, wo_t, heads, obuf)
        rows = pl.ds(ROWS * t, ROWS)
        for d in range(1, n_col):
            peer = at_col(d)
            remote(obuf.at[peer, rows], res.at[col, rows],
                   o_send.at[d - 1], o_recv.at[d - 1], {'col': peer}).start()
        return carry

    lax.fori_loop(0, n_pair, late_body, 0)

    mine = pltpu.make_async_copy(obuf.at[col], res.at[col], own_sem)
    mine.start()
    for c in b1 + zc[0] + zc[1] + b2[0] + b2[1] + b3[0] + b3[1]:
        c.wait_send()
    for d in range(1, n_col):
        peer = at_col(d)
        whole = remote(obuf.at[peer], res.at[col], o_send.at[d - 1], o_recv.at[d - 1], {'col': peer})
        whole.wait_send()
        whole.wait_recv()
    mine.wait()


def solution(mesh):
    n_col = mesh.shape['col']
    n_row = mesh.shape['row']
    tile_spec = P(('dp', 'row'), 'col', None)
    vmem = pl.BlockSpec(memory_space=pltpu.VMEM)

    def per_device(pair_tile, res_mask, ln_gamma, ln_beta, w_q, w_k, w_v, w_b, w_g, w_o):
        row_len, col_len, chan = pair_tile.shape
        heads = w_b.shape[1]
        hd = chan // heads
        n = res_mask.shape[0]
        own = row_len // n_col
        hc = chan // 2
        lanes = 2 * col_len
        dma = pltpu.SemaphoreType.DMA
        res = pl.pallas_call(
            functools.partial(attn_kernel, n_col, n_row),
            in_specs=[vmem] * 10,
            out_specs=pl.BlockSpec(memory_space=pl.ANY),
            out_shape=jax.ShapeDtypeStruct((n_col, own, hc, lanes), BF16),
            scratch_shapes=[
                pltpu.VMEM((heads, col_len, row_len), BF16),
                pltpu.VMEM((row_len, hc, lanes), BF16),
                pltpu.VMEM((n_col, own, hc, lanes), BF16),
                pltpu.VMEM((n_row, heads, n, row_len), BF16),
                pltpu.VMEM((heads, n, n), F32),
                pltpu.VMEM((n, row_len), F32),
                pltpu.VMEM((own, chan, n), F32),
                pltpu.VMEM((own * heads, chan, n), BF16),
                pltpu.VMEM((own, n, chan), BF16),
                pltpu.VMEM((own * heads, hd, n), BF16),
                pltpu.VMEM((own * heads, hd, n), F32),
                pltpu.VMEM((2 * ROWS, n, n), F32),
                pltpu.VMEM((2 * ROWS, 1, n), F32),
                pltpu.VMEM((own * heads, hd, n), BF16),
                pltpu.VMEM((n_col, own, hc, lanes), BF16),
                dma((n_col - 1,)), dma((n_col - 1,)), dma((2, n_col - 1)), dma((2, n_col - 1)),
                dma((heads // 2, n_row - 1)), dma((heads // 2, n_row - 1)),
                dma((heads // 2, n_row)), dma((heads // 2, n_row)),
                dma((n_col - 1,)), dma((n_col - 1,)), dma,
            ],
            compiler_params=pltpu.CompilerParams(
                collective_id=0, has_side_effects=True, vmem_limit_bytes=52 << 20),
            name='attention',
        )(jnp.transpose(pair_tile, (1, 2, 0)), res_mask.reshape(1, n), ln_gamma.reshape(1, chan),
          ln_beta.reshape(1, chan), w_q, w_k, w_v, w_g, w_b.T, w_o)

        out = pl.pallas_call(
            unpack_kernel,
            in_specs=[vmem],
            out_specs=vmem,
            out_shape=jax.ShapeDtypeStruct((col_len, chan, row_len), BF16),
            name='unpack',
        )(res.reshape(row_len, hc, lanes))
        return jnp.transpose(out, (2, 0, 1))

    return jax.shard_map(per_device, mesh=mesh,
                         in_specs=(tile_spec, P('dp'), P(), P(), P(), P(), P(), P(), P(), P()),
                         out_specs=tile_spec, check_vma=False)
```

```python
import functools

import jax
import jax.numpy as jnp
from jax import lax
from jax.experimental import pallas as pl
from jax.experimental.pallas import tpu as pltpu
from jax.sharding import PartitionSpec as P

LN_EPS = 1e-5
F32 = jnp.float32
BF16 = jnp.bfloat16
MESH = pl.DeviceIdType.MESH

KEYS = 64
TILE = 256


def column(row, lanes):
    return jnp.broadcast_to(row, (lanes, row.shape[-1])).T


def layer_norm(z, gamma, beta, axis):
    mean = jnp.mean(z, axis=axis, keepdims=True)
    cen = z - mean
    var = jnp.mean(cen * cen, axis=axis, keepdims=True)
    return (cen * lax.rsqrt(var + LN_EPS) * gamma + beta).astype(BF16)


def tile_bias(zin, wb_t, gamma, beta, bt):
    n_key, chan, n_q = zin.shape
    heads = bt.shape[0]
    group = 16
    wide = jnp.concatenate([wb_t, wb_t], axis=1)
    wide = jnp.concatenate([wide] * (group // 2), axis=1)
    rows = jnp.concatenate([jnp.broadcast_to(wide[h:h + 1], (group, group * chan)) for h in range(heads)], axis=0)
    own = lax.broadcasted_iota(jnp.int32, rows.shape, 0) % group
    src = lax.broadcasted_iota(jnp.int32, rows.shape, 1) // chan
    big = jnp.where(own == src, rows, 0.0).astype(BF16)

    def body(g, carry):
        start = pl.multiple_of(g * group, group)
        normed = layer_norm(zin[pl.ds(start, group)].astype(F32), gamma[None], beta[None], 1)
        out = jnp.dot(big, normed.reshape(group * chan, n_q), preferred_element_type=F32)
        for h in range(heads):
            bt[h, pl.ds(start, group), :] = out[h * group:(h + 1) * group].astype(BF16)
        return carry

    lax.fori_loop(0, n_key // group, body, 0)


def to_rows(zin, zt):
    n_key, chan, _ = zin.shape
    hc = chan // 2
    for s in range(0, hc, 16):
        a = jnp.swapaxes(zin[:, s:s + 16, :].astype(F32), 0, 1)
        b = jnp.swapaxes(zin[:, hc + s:hc + s + 16, :].astype(F32), 0, 1)
        c = jnp.concatenate([a, b], axis=1)
        c = jnp.stack([c[i].T for i in range(16)], axis=0)
        zt[:, s:s + 16, :] = jnp.swapaxes(c, 0, 1).astype(BF16)


def unpack_kernel(r, out):
    n_key = out.shape[0]
    pairs = r.shape[1]
    c = jnp.swapaxes(r[...].astype(F32), 0, 1)
    c = [c[i].T for i in range(pairs)]
    for half in range(2):
        x = jnp.stack([y[half * n_key:(half + 1) * n_key] for y in c], axis=0)
        out[:, half] = jnp.swapaxes(x, 0, 1).astype(BF16)


def project(r, zbuf, w_t, gamma, beta, heads, zr, qz, kr, vr, gr):
    n_src, _, hc, lanes = zbuf.shape
    chan = 2 * hc
    half = lanes // 2
    n = n_src * half
    hd = chan // heads
    low = lax.broadcasted_iota(jnp.int32, (hc, lanes), 1) < half
    cols = []
    for x in range(n_src // 2):
        a = zbuf[2 * x, r].astype(F32)
        b = zbuf[2 * x + 1, r].astype(F32)
        top = jnp.where(low, a, pltpu.roll(b, half, 1))
        bot = jnp.where(low, pltpu.roll(a, half, 1), b)
        cols.append(jnp.concatenate([top, bot], axis=0))
    z = jnp.concatenate(cols, axis=1)
    zr[r] = z
    proj = jnp.dot(w_t, layer_norm(z, gamma, beta, 0), preferred_element_type=F32)
    q_t = (proj[:chan] * hd ** -0.5).astype(BF16)
    for h in range(heads):
        parts = []
        if h > 0:
            parts.append(jnp.zeros((h * hd, n), BF16))
        parts.append(q_t[h * hd:(h + 1) * hd])
        if h < heads - 1:
            parts.append(jnp.zeros(((heads - 1 - h) * hd, n), BF16))
        qz[r * heads + h] = jnp.concatenate(parts, axis=0)
        vr[r * heads + h] = proj[2 * chan + h * hd:2 * chan + (h + 1) * hd].astype(BF16)
        gr[r * heads + h] = jax.nn.sigmoid(proj[3 * chan + h * hd:3 * chan + (h + 1) * hd])
    kr[r] = proj[chan:2 * chan].T.astype(BF16)


class Logits:
    def __init__(self, slot, row, head, heads, bias, qz, kr, sref, mref):
        self.slot, self.head, self.bias, self.sref, self.mref = slot, head, bias, sref, mref
        self.value = jnp.dot(kr[row], qz[row * heads + head], preferred_element_type=F32)
        self.top = None
        self.done = 0

    def advance(self):
        n = self.sref.shape[-1]
        if self.done == n:
            return
        sl = slice(self.done, self.done + KEYS)
        self.done += KEYS
        part = self.value[sl] + self.bias[self.head, sl, :]
        self.sref[self.slot, sl, :] = part
        top = jnp.max(part.reshape(KEYS // 8, 8, n), axis=0)
        self.top = top if self.top is None else jnp.maximum(self.top, top)

    def end(self):
        while self.done < self.sref.shape[-1]:
            self.advance()
        self.mref[self.slot] = jnp.max(self.top, axis=0, keepdims=True)


def step(s, early, own, heads, bias, qz, kr, vr, gr, sref, mref, gat, do_ex=True):
    n = sref.shape[-1]
    hh = heads // 2
    nxt = s + 1 if isinstance(s, int) else jnp.minimum(s + 1, own - 1)

    def place(at, i):
        split = at < 2 * early
        row = jnp.where(split, (at % early) * 2 + i // hh, at)
        head = jnp.where(split, at // early + hh * (i % hh), i)
        return row, head

    pending = None
    for i in range(heads):
        row, head = place(nxt, i)
        logits = Logits(i, row, head, heads, bias, qz, kr, sref, mref)
        if do_ex:
            row, head = place(s, i)
            idx = row * heads + head
            v = vr[idx]
            g = gr[idx]
            outs = []
            for q0 in range(0, n, TILE):
                qs = slice(q0, q0 + TILE)
                peak = jnp.broadcast_to(mref[i, :, qs], (8, TILE))[None]
                total = jnp.zeros((8, TILE), F32)
                acc = None
                for k0 in range(0, n, TILE):
                    parts = []
                    for k1 in range(k0, k0 + TILE, KEYS):
                        p = jnp.exp(sref[i, k1:k1 + KEYS, qs].reshape(KEYS // 8, 8, TILE) - peak)
                        total = total + jnp.sum(p, axis=0)
                        parts.append(p.reshape(KEYS, TILE).astype(BF16))
                        if pending is not None:
                            pending.advance()
                    d = jnp.dot(v[:, k0:k0 + TILE], jnp.concatenate(parts, axis=0), preferred_element_type=F32)
                    acc = d if acc is None else acc + d
                outs.append((g[:, qs] * (acc / jnp.sum(total, axis=0, keepdims=True))).astype(BF16))
            gat[idx] = jnp.concatenate(outs, axis=1)
        if pending is not None:
            pending.end()
        pending = logits
    pending.end()


def finish(r, zr, gat, wo_t, heads, obuf):
    n_src, _, hc, lanes = obuf.shape
    half = lanes // 2
    low = lax.broadcasted_iota(jnp.int32, (hc, lanes), 1) < half
    gated = jnp.concatenate([gat[r * heads + h] for h in range(heads)], axis=0)
    o = zr[r] + jnp.dot(wo_t, gated, preferred_element_type=F32)
    for x in range(n_src // 2):
        top = o[:hc, x * lanes:(x + 1) * lanes]
        bot = o[hc:, x * lanes:(x + 1) * lanes]
        obuf[2 * x, r] = jnp.where(low, top, pltpu.roll(bot, half, 1)).astype(BF16)
        obuf[2 * x + 1, r] = jnp.where(low, pltpu.roll(top, half, 1), bot).astype(BF16)


def attn_kernel(n_col, n_row, zin_h, mask_h, gamma_h, beta_h, wq_h, wk_h, wv_h, wg_h, wb_h, wo_h, res,
                zin, mask, gamma_row, beta_row, w_q, w_k, w_v, w_g, wb_t, w_o,
                bt, zt, zbuf, ball, bias, kb, zr, qz, kr, vr, gr, sref, mref, gat, obuf, w_t, wo_t, affine,
                in_sem, b1_send, b1_recv, z_send, z_recv, b2_send, b2_recv, b3_send, b3_recv,
                o_send, o_recv, own_sem):
    col = lax.axis_index('col')
    row = lax.axis_index('row')
    core = lax.rem(col, 2)
    mate = col + 1 - 2 * core
    heads, cols, strip = bt.shape
    hh = heads // 2
    own = zbuf.shape[1]
    n = sref.shape[-1]
    n_part = z_send.shape[0]
    part = own // n_part
    early = own // 4

    def at_col(d):
        return lax.rem(col + d, n_col)

    def at_row(d):
        return lax.rem(row + d, n_row)

    def remote(src, dst, send, recv, where):
        return pltpu.make_async_remote_copy(src_ref=src, dst_ref=dst, send_sem=send, recv_sem=recv,
                                            device_id=where, device_id_type=MESH)

    loads = [pltpu.make_async_copy(src, dst, in_sem.at[i]) for i, (src, dst) in enumerate((
        (gamma_h, gamma_row), (beta_h, beta_row), (wb_h, wb_t), (zin_h, zin), (mask_h, mask),
        (wq_h, w_q), (wk_h, w_k), (wv_h, w_v), (wg_h, w_g), (wo_h, w_o)))]
    for c in loads:
        c.start()

    barrier = pltpu.get_barrier_semaphore()
    for d in range(1, n_col):
        pl.semaphore_signal(barrier, inc=1, device_id={'col': at_col(d)}, device_id_type=MESH)
    for d in range(1, n_row):
        pl.semaphore_signal(barrier, inc=1, device_id={'row': at_row(d)}, device_id_type=MESH)

    for c in loads[:4]:
        c.wait()
    ga = column(gamma_row[...], strip)
    be = column(beta_row[...], strip)
    tile_bias(zin, wb_t[...].astype(F32), ga, be, bt)
    pl.semaphore_wait(barrier, n_col + n_row - 2)

    def keys_of(c):
        return pl.ds(pl.multiple_of(c * cols, cols), cols)

    def first(e, d):
        peer = at_col(d)
        head = lax.rem(peer, 2) * hh + e
        return remote(bt.at[head], ball.at[row, head, keys_of(col), :],
                      b1_send.at[e, d - 1], b1_recv.at[e, d - 1], {'col': peer})

    def second(e, src, c, d):
        head = core * hh + e
        return remote(src, ball.at[row, head, keys_of(c), :],
                      b2_send.at[e, d - 1], b2_recv.at[e, d - 1], {'row': at_row(d)})

    for e in range(hh):
        for d in range(1, n_col):
            first(e, d).start()
        if e == 0:
            for d in range(1, n_row):
                second(e, bt.at[core * hh + e], col, d).start()

    def rows_out(q, d):
        peer = at_col(d)
        return remote(zt.at[pl.ds(peer * own + q * part, part)], zbuf.at[col, pl.ds(q * part, part)],
                      z_send.at[q, d - 1], z_recv.at[q, d - 1], {'col': peer})

    to_rows(zin, zt)
    for q in range(n_part):
        for d in range(1, n_col):
            rows_out(q, d).start()

    for e in range(hh):
        head = core * hh + e
        if e > 0:
            for d in range(1, n_row):
                second(e, bt.at[head], col, d).start()
        ball[row, head, keys_of(col), :] = bt[head]
        for d in range(1, n_col):
            first(e, d).wait_recv()
            src = lax.rem(col + n_col - d, n_col)
            for f in range(1, n_row):
                second(e, ball.at[row, head, keys_of(src), :], src, f).start()

    def third(e, d):
        head = core * hh + e
        from_row = lax.rem(row + n_row - d, n_row)
        return remote(ball.at[from_row, head], ball.at[from_row, head],
                      b3_send.at[e, d], b3_recv.at[e, d], {'col': mate})

    def whole_second(e, d):
        head = core * hh + e
        return remote(ball.at[row, head], ball.at[row, head],
                      b2_send.at[e, d - 1], b2_recv.at[e, d - 1], {'row': at_row(d)})

    def pass_on(e):
        for d in range(n_row):
            if d > 0:
                whole_second(e, d).wait_recv()
            third(e, d).start()

    def take_bias(e):
        for d in range(n_row):
            third(e, d).wait_recv()
        for h in range(e, heads, hh):
            for r in range(n_row):
                bias[h, :, r * strip:(r + 1) * strip] = ball[r, h].astype(F32) + kb[...]

    for c in loads[4:]:
        c.wait()
    kb[...] = column(jnp.where(mask[...] > 0, 0.0, -1e9).astype(F32), strip)
    w_t[...] = jnp.concatenate([w[...].astype(F32).T for w in (w_q, w_k, w_v, w_g)], axis=0).astype(BF16)
    wo_t[...] = w_o[...].astype(F32).T.astype(BF16)
    affine[0] = ga
    affine[1] = be
    zbuf[col] = zt[pl.ds(col * own, own)]

    def take_rows(q):
        for d in range(1, n_col):
            rows_out(q, d).wait_recv()
        wide = [jnp.concatenate([affine[i]] * (n // strip), axis=1) for i in range(2)]

        def body(r, carry):
            project(r, zbuf, w_t[...], wide[0], wide[1], heads, zr, qz, kr, vr, gr)
            return carry

        lax.fori_loop(q * part, (q + 1) * part, body, 0)

    run = functools.partial(step, early=early, own=own, heads=heads, bias=bias, qz=qz, kr=kr, vr=vr,
                            gr=gr, sref=sref, mref=mref, gat=gat)

    def give_row(r):
        finish(r, zr, gat, wo_t[...], heads, obuf)
        for d in range(1, n_col):
            peer = at_col(d)
            remote(obuf.at[peer, r], res.at[col, r], o_send.at[d - 1], o_recv.at[d - 1], {'col': peer}).start()

    take_rows(0)
    pass_on(0)
    take_bias(0)
    run(-1, do_ex=False)

    def body(s, carry):
        @pl.when(s == 0)
        def _():
            take_rows(1)

        @pl.when(s == 1)
        def _():
            pass_on(1)

        @pl.when(s == early - 2)
        def _():
            take_bias(1)

        @pl.when(s == early)
        def _():
            take_rows(2)

        @pl.when(s == early + 2)
        def _():
            take_rows(3)

        run(s)

        @pl.when((s >= early) & (s < 2 * early))
        def _():
            for i in range(2):
                give_row((s - early) * 2 + i)

        @pl.when(s >= 2 * early)
        def _():
            give_row(s)

        return carry

    lax.fori_loop(0, own, body, 0)

    mine = pltpu.make_async_copy(obuf.at[col], res.at[col], own_sem)
    mine.start()
    for e in range(hh):
        for d in range(1, n_col):
            first(e, d).wait_send()
        for d in range(1, n_row):
            whole_second(e, d).wait_send()
        for d in range(n_row):
            third(e, d).wait_send()
    for q in range(n_part):
        for d in range(1, n_col):
            rows_out(q, d).wait_send()
    for d in range(1, n_col):
        peer = at_col(d)
        whole = remote(obuf.at[peer], res.at[col], o_send.at[d - 1], o_recv.at[d - 1], {'col': peer})
        whole.wait_send()
        whole.wait_recv()
    mine.wait()


def solution(mesh):
    n_col = mesh.shape['col']
    n_row = mesh.shape['row']
    tile_spec = P(('dp', 'row'), 'col', None)
    hbm = pl.BlockSpec(memory_space=pltpu.HBM)
    n_part = 4

    def per_device(pair_tile, res_mask, ln_gamma, ln_beta, w_q, w_k, w_v, w_b, w_g, w_o):
        row_len, col_len, chan = pair_tile.shape
        heads = w_b.shape[1]
        hd = chan // heads
        n = res_mask.shape[0]
        own = row_len // n_col
        hc = chan // 2
        lanes = 2 * col_len
        dma = pltpu.SemaphoreType.DMA
        res = pl.pallas_call(
            functools.partial(attn_kernel, n_col, n_row),
            in_specs=[hbm] * 10,
            out_specs=hbm,
            out_shape=jax.ShapeDtypeStruct((n_col, own, hc, lanes), BF16),
            scratch_shapes=[
                pltpu.VMEM((col_len, chan, row_len), BF16),
                pltpu.VMEM((1, n), res_mask.dtype),
                pltpu.VMEM((1, chan), F32),
                pltpu.VMEM((1, chan), F32),
                pltpu.VMEM(w_q.shape, BF16),
                pltpu.VMEM(w_k.shape, BF16),
                pltpu.VMEM(w_v.shape, BF16),
                pltpu.VMEM(w_g.shape, BF16),
                pltpu.VMEM((heads, chan), BF16),
                pltpu.VMEM(w_o.shape, BF16),
                pltpu.VMEM((heads, col_len, row_len), BF16),
                pltpu.VMEM((row_len, hc, lanes), BF16),
                pltpu.VMEM((n_col, own, hc, lanes), BF16),
                pltpu.VMEM((n_row, heads, n, row_len), BF16),
                pltpu.VMEM((heads, n, n), F32),
                pltpu.VMEM((n, row_len), F32),
                pltpu.VMEM((own, chan, n), F32),
                pltpu.VMEM((own * heads, chan, n), BF16),
                pltpu.VMEM((own, n, chan), BF16),
                pltpu.VMEM((own * heads, hd, n), BF16),
                pltpu.VMEM((own * heads, hd, n), F32),
                pltpu.VMEM((heads, n, n), F32),
                pltpu.VMEM((heads, 1, n), F32),
                pltpu.VMEM((own * heads, hd, n), BF16),
                pltpu.VMEM((n_col, own, hc, lanes), BF16),
                pltpu.VMEM((4 * chan, chan), BF16),
                pltpu.VMEM((chan, chan), BF16),
                pltpu.VMEM((2, chan, row_len), F32),
                dma((10,)),
                dma((heads // 2, n_col - 1)), dma((heads // 2, n_col - 1)),
                dma((n_part, n_col - 1)), dma((n_part, n_col - 1)),
                dma((heads // 2, n_row - 1)), dma((heads // 2, n_row - 1)),
                dma((heads // 2, n_row)), dma((heads // 2, n_row)),
                dma((n_col - 1,)), dma((n_col - 1,)), dma,
            ],
            compiler_params=pltpu.CompilerParams(
                collective_id=0, has_side_effects=True, vmem_limit_bytes=56 << 20),
            name='attention',
        )(jnp.transpose(pair_tile, (1, 2, 0)), res_mask.reshape(1, n), ln_gamma.reshape(1, chan),
          ln_beta.reshape(1, chan), w_q, w_k, w_v, w_g, w_b.T, w_o)

        pairs = 16
        out = pl.pallas_call(
            unpack_kernel,
            grid=(hc // pairs,),
            in_specs=[pl.BlockSpec((row_len, pairs, lanes), lambda i: (0, i, 0))],
            out_specs=pl.BlockSpec((col_len, 2, pairs, row_len), lambda i: (0, 0, i, 0)),
            out_shape=jax.ShapeDtypeStruct((col_len, 2, hc, row_len), BF16),
            name='unpack',
        )(res.reshape(row_len, hc, lanes)).reshape(col_len, chan, row_len)
        return jnp.transpose(out, (2, 0, 1))

    return jax.shard_map(per_device, mesh=mesh,
                         in_specs=(tile_spec, P('dp'), P(), P(), P(), P(), P(), P(), P(), P()),
                         out_specs=tile_spec, check_vma=False)
```

```python
import functools

import jax
import jax.numpy as jnp
from jax import lax
from jax.experimental import pallas as pl
from jax.experimental.pallas import tpu as pltpu
from jax.sharding import PartitionSpec as P

LN_EPS = 1e-5
F32 = jnp.float32
BF16 = jnp.bfloat16
MESH = pl.DeviceIdType.MESH

KEYS = 64
TILE = 256


def column(row, lanes):
    return jnp.broadcast_to(row, (lanes, row.shape[-1])).T


def layer_norm(z, gamma, beta, axis):
    mean = jnp.mean(z, axis=axis, keepdims=True)
    cen = z - mean
    var = jnp.mean(cen * cen, axis=axis, keepdims=True)
    return (cen * lax.rsqrt(var + LN_EPS) * gamma + beta).astype(BF16)


def tile_bias(zin, wb_t, gamma, beta, bt):
    n_key, chan, n_q = zin.shape
    heads = bt.shape[0]
    group = 16
    wide = jnp.concatenate([wb_t, wb_t], axis=1)
    wide = jnp.concatenate([wide] * (group // 2), axis=1)
    rows = jnp.concatenate([jnp.broadcast_to(wide[h:h + 1], (group, group * chan)) for h in range(heads)], axis=0)
    own = lax.broadcasted_iota(jnp.int32, rows.shape, 0) % group
    src = lax.broadcasted_iota(jnp.int32, rows.shape, 1) // chan
    big = jnp.where(own == src, rows, 0.0).astype(BF16)

    def body(g, carry):
        start = pl.multiple_of(g * group, group)
        normed = layer_norm(zin[pl.ds(start, group)].astype(F32), gamma[None], beta[None], 1)
        out = jnp.dot(big, normed.reshape(group * chan, n_q), preferred_element_type=F32)
        for h in range(heads):
            bt[h, pl.ds(start, group), :] = out[h * group:(h + 1) * group].astype(BF16)
        return carry

    lax.fori_loop(0, n_key // group, body, 0)


def to_rows(zin, zt):
    n_key, chan, _ = zin.shape
    hc = chan // 2
    for s in range(0, hc, 16):
        a = jnp.swapaxes(zin[:, s:s + 16, :].astype(F32), 0, 1)
        b = jnp.swapaxes(zin[:, hc + s:hc + s + 16, :].astype(F32), 0, 1)
        c = jnp.concatenate([a, b], axis=1)
        c = jnp.stack([c[i].T for i in range(16)], axis=0)
        zt[:, s:s + 16, :] = jnp.swapaxes(c, 0, 1).astype(BF16)


def unpack_kernel(r, out):
    n_key = out.shape[0]
    pairs = r.shape[1]
    c = jnp.swapaxes(r[...].astype(F32), 0, 1)
    c = [c[i].T for i in range(pairs)]
    for half in range(2):
        x = jnp.stack([y[half * n_key:(half + 1) * n_key] for y in c], axis=0)
        out[:, half] = jnp.swapaxes(x, 0, 1).astype(BF16)


def project(r, zbuf, w_t, gamma, beta, heads, zr, qz, kr, vr, gr):
    n_src, _, hc, lanes = zbuf.shape
    chan = 2 * hc
    half = lanes // 2
    n = n_src * half
    hd = chan // heads
    low = lax.broadcasted_iota(jnp.int32, (hc, lanes), 1) < half
    cols = []
    for x in range(n_src // 2):
        a = zbuf[2 * x, r].astype(F32)
        b = zbuf[2 * x + 1, r].astype(F32)
        top = jnp.where(low, a, pltpu.roll(b, half, 1))
        bot = jnp.where(low, pltpu.roll(a, half, 1), b)
        cols.append(jnp.concatenate([top, bot], axis=0))
    z = jnp.concatenate(cols, axis=1)
    zr[r] = z
    proj = jnp.dot(w_t, layer_norm(z, gamma, beta, 0), preferred_element_type=F32)
    q_t = (proj[:chan] * hd ** -0.5).astype(BF16)
    for h in range(heads):
        parts = []
        if h > 0:
            parts.append(jnp.zeros((h * hd, n), BF16))
        parts.append(q_t[h * hd:(h + 1) * hd])
        if h < heads - 1:
            parts.append(jnp.zeros(((heads - 1 - h) * hd, n), BF16))
        qz[r * heads + h] = jnp.concatenate(parts, axis=0)
        vr[r * heads + h] = proj[2 * chan + h * hd:2 * chan + (h + 1) * hd].astype(BF16)
        gr[r * heads + h] = jax.nn.sigmoid(proj[3 * chan + h * hd:3 * chan + (h + 1) * hd])
    kr[r] = proj[chan:2 * chan].T.astype(BF16)


class Logits:
    def __init__(self, slot, row, head, heads, bias, qz, kr, sref, mref):
        self.slot, self.head, self.bias, self.sref, self.mref = slot, head, bias, sref, mref
        self.value = jnp.dot(kr[row], qz[row * heads + head], preferred_element_type=F32)
        self.top = None
        self.done = 0

    def advance(self):
        n = self.sref.shape[-1]
        if self.done == n:
            return
        sl = slice(self.done, self.done + KEYS)
        self.done += KEYS
        part = self.value[sl] + self.bias[self.head, sl, :]
        self.sref[self.slot, sl, :] = part
        top = jnp.max(part.reshape(KEYS // 8, 8, n), axis=0)
        self.top = top if self.top is None else jnp.maximum(self.top, top)

    def end(self):
        while self.done < self.sref.shape[-1]:
            self.advance()
        self.mref[self.slot] = jnp.max(self.top, axis=0, keepdims=True)


def step(s, own, heads, bias, qz, kr, vr, gr, sref, mref, gat, do_ex=True):
    n = sref.shape[-1]
    nxt = s + 1 if isinstance(s, int) else jnp.minimum(s + 1, own - 1)
    pending = None
    for i in range(heads):
        logits = Logits(i, nxt, i, heads, bias, qz, kr, sref, mref)
        if do_ex:
            idx = s * heads + i
            v = vr[idx]
            g = gr[idx]
            outs = []
            for q0 in range(0, n, TILE):
                qs = slice(q0, q0 + TILE)
                peak = jnp.broadcast_to(mref[i, :, qs], (8, TILE))[None]
                total = jnp.zeros((8, TILE), F32)
                acc = None
                for k0 in range(0, n, TILE):
                    parts = []
                    for k1 in range(k0, k0 + TILE, KEYS):
                        p = jnp.exp(sref[i, k1:k1 + KEYS, qs].reshape(KEYS // 8, 8, TILE) - peak)
                        total = total + jnp.sum(p, axis=0)
                        parts.append(p.reshape(KEYS, TILE).astype(BF16))
                        if pending is not None:
                            pending.advance()
                    d = jnp.dot(v[:, k0:k0 + TILE], jnp.concatenate(parts, axis=0), preferred_element_type=F32)
                    acc = d if acc is None else acc + d
                outs.append((g[:, qs] * (acc / jnp.sum(total, axis=0, keepdims=True))).astype(BF16))
            gat[idx] = jnp.concatenate(outs, axis=1)
        if pending is not None:
            pending.end()
        pending = logits
    pending.end()


def finish(r, zr, gat, wo_t, heads, obuf):
    n_src, _, hc, lanes = obuf.shape
    half = lanes // 2
    low = lax.broadcasted_iota(jnp.int32, (hc, lanes), 1) < half
    gated = jnp.concatenate([gat[r * heads + h] for h in range(heads)], axis=0)
    o = zr[r] + jnp.dot(wo_t, gated, preferred_element_type=F32)
    for x in range(n_src // 2):
        top = o[:hc, x * lanes:(x + 1) * lanes]
        bot = o[hc:, x * lanes:(x + 1) * lanes]
        obuf[2 * x, r] = jnp.where(low, top, pltpu.roll(bot, half, 1)).astype(BF16)
        obuf[2 * x + 1, r] = jnp.where(low, pltpu.roll(top, half, 1), bot).astype(BF16)


def attn_kernel(n_col, n_row, zin_h, mask_h, gamma_h, beta_h, wq_h, wk_h, wv_h, wg_h, wb_h, wo_h, res,
                zin, mask, gamma_row, beta_row, w_q, w_k, w_v, w_g, wb_t, w_o,
                bt, zt, zbuf, ball, bias, kb, zr, qz, kr, vr, gr, sref, mref, gat, obuf, w_t, wo_t, affine,
                in_sem, b1_send, b1_recv, z_send, z_recv, b2_send, b2_recv, b3_send, b3_recv,
                o_send, o_recv, own_sem):
    col = lax.axis_index('col')
    row = lax.axis_index('row')
    core = lax.rem(col, 2)
    mate = col + 1 - 2 * core
    heads, cols, strip = bt.shape
    hh = heads // 2
    own = zbuf.shape[1]
    n = sref.shape[-1]
    n_part = z_send.shape[0]
    part = own // n_part

    def at_col(d):
        return lax.rem(col + d, n_col)

    def at_row(d):
        return lax.rem(row + d, n_row)

    def remote(src, dst, send, recv, where):
        return pltpu.make_async_remote_copy(src_ref=src, dst_ref=dst, send_sem=send, recv_sem=recv,
                                            device_id=where, device_id_type=MESH)

    loads = [pltpu.make_async_copy(src, dst, in_sem.at[i]) for i, (src, dst) in enumerate((
        (gamma_h, gamma_row), (beta_h, beta_row), (wb_h, wb_t), (zin_h, zin), (mask_h, mask),
        (wq_h, w_q), (wk_h, w_k), (wv_h, w_v), (wg_h, w_g), (wo_h, w_o)))]
    for c in loads:
        c.start()

    barrier = pltpu.get_barrier_semaphore()
    for d in range(1, n_col):
        pl.semaphore_signal(barrier, inc=1, device_id={'col': at_col(d)}, device_id_type=MESH)
    for d in range(1, n_row):
        pl.semaphore_signal(barrier, inc=1, device_id={'row': at_row(d)}, device_id_type=MESH)

    for c in loads[:4]:
        c.wait()
    ga = column(gamma_row[...], strip)
    be = column(beta_row[...], strip)
    tile_bias(zin, wb_t[...].astype(F32), ga, be, bt)
    pl.semaphore_wait(barrier, n_col + n_row - 2)

    def keys_of(c):
        return pl.ds(pl.multiple_of(c * cols, cols), cols)

    def first(e, d):
        peer = at_col(d)
        head = lax.rem(peer, 2) * hh + e
        return remote(bt.at[head], ball.at[row, head, keys_of(col), :],
                      b1_send.at[e, d - 1], b1_recv.at[e, d - 1], {'col': peer})

    def second(e, src, c, d):
        head = core * hh + e
        return remote(src, ball.at[row, head, keys_of(c), :],
                      b2_send.at[e, d - 1], b2_recv.at[e, d - 1], {'row': at_row(d)})

    for e in range(hh):
        for d in range(1, n_col):
            first(e, d).start()
        if e == 0:
            for d in range(1, n_row):
                second(e, bt.at[core * hh + e], col, d).start()

    def rows_out(q, d):
        peer = at_col(d)
        return remote(zt.at[pl.ds(peer * own + q * part, part)], zbuf.at[col, pl.ds(q * part, part)],
                      z_send.at[q, d - 1], z_recv.at[q, d - 1], {'col': peer})

    to_rows(zin, zt)
    for q in range(n_part):
        for d in range(1, n_col):
            rows_out(q, d).start()

    for e in range(hh):
        head = core * hh + e
        if e > 0:
            for d in range(1, n_row):
                second(e, bt.at[head], col, d).start()
        ball[row, head, keys_of(col), :] = bt[head]
        for d in range(1, n_col):
            first(e, d).wait_recv()
            src = lax.rem(col + n_col - d, n_col)
            for f in range(1, n_row):
                second(e, ball.at[row, head, keys_of(src), :], src, f).start()

    def third(e, d):
        head = core * hh + e
        from_row = lax.rem(row + n_row - d, n_row)
        return remote(ball.at[from_row, head], ball.at[from_row, head],
                      b3_send.at[e, d], b3_recv.at[e, d], {'col': mate})

    def whole_second(e, d):
        head = core * hh + e
        return remote(ball.at[row, head], ball.at[row, head],
                      b2_send.at[e, d - 1], b2_recv.at[e, d - 1], {'row': at_row(d)})

    def pass_on(e):
        for d in range(n_row):
            if d > 0:
                whole_second(e, d).wait_recv()
            third(e, d).start()

    def widen(h):
        for r in range(n_row):
            bias[h, :, r * strip:(r + 1) * strip] = ball[r, h].astype(F32) + kb[...]

    for c in loads[4:]:
        c.wait()
    kb[...] = column(jnp.where(mask[...] > 0, 0.0, -1e9).astype(F32), strip)
    w_t[...] = jnp.concatenate([w[...].astype(F32).T for w in (w_q, w_k, w_v, w_g)], axis=0).astype(BF16)
    wo_t[...] = w_o[...].astype(F32).T.astype(BF16)
    affine[0] = ga
    affine[1] = be
    zbuf[col] = zt[pl.ds(col * own, own)]

    def take_rows(q):
        for d in range(1, n_col):
            rows_out(q, d).wait_recv()
        wide = [jnp.concatenate([affine[i]] * (n // strip), axis=1) for i in range(2)]

        def body(r, carry):
            project(r, zbuf, w_t[...], wide[0], wide[1], heads, zr, qz, kr, vr, gr)
            return carry

        lax.fori_loop(q * part, (q + 1) * part, body, 0)

    run = functools.partial(step, own=own, heads=heads, bias=bias, qz=qz, kr=kr, vr=vr,
                            gr=gr, sref=sref, mref=mref, gat=gat)

    def make_row(r):
        finish(r, zr, gat, wo_t[...], heads, obuf)

    def give_row(r):
        for d in range(1, n_col):
            peer = at_col(d)
            remote(obuf.at[peer, r], res.at[col, r], o_send.at[d - 1], o_recv.at[d - 1], {'col': peer}).start()

    for q in range(n_part):
        if q == n_part - 1:
            pass_on(0)
        take_rows(q)
    pass_on(1)
    for e in range(hh):
        widen(core * hh + e)
    for e in range(hh):
        for d in range(n_row):
            third(e, d).wait_recv()
    for e in range(hh):
        widen((1 - core) * hh + e)

    run(-1, do_ex=False)
    run(0)

    def body(s, carry):
        make_row(s - 1)
        run(s)
        give_row(s - 1)
        return carry

    lax.fori_loop(1, own, body, 0)
    make_row(own - 1)
    give_row(own - 1)

    mine = pltpu.make_async_copy(obuf.at[col], res.at[col], own_sem)
    mine.start()
    for e in range(hh):
        for d in range(1, n_col):
            first(e, d).wait_send()
        for d in range(1, n_row):
            whole_second(e, d).wait_send()
        for d in range(n_row):
            third(e, d).wait_send()
    for q in range(n_part):
        for d in range(1, n_col):
            rows_out(q, d).wait_send()
    for d in range(1, n_col):
        peer = at_col(d)
        whole = remote(obuf.at[peer], res.at[col], o_send.at[d - 1], o_recv.at[d - 1], {'col': peer})
        whole.wait_send()
        whole.wait_recv()
    mine.wait()


def solution(mesh):
    n_col = mesh.shape['col']
    n_row = mesh.shape['row']
    tile_spec = P(('dp', 'row'), 'col', None)
    hbm = pl.BlockSpec(memory_space=pltpu.HBM)
    n_part = 4

    def per_device(pair_tile, res_mask, ln_gamma, ln_beta, w_q, w_k, w_v, w_b, w_g, w_o):
        row_len, col_len, chan = pair_tile.shape
        heads = w_b.shape[1]
        hd = chan // heads
        n = res_mask.shape[0]
        own = row_len // n_col
        hc = chan // 2
        lanes = 2 * col_len
        dma = pltpu.SemaphoreType.DMA
        res = pl.pallas_call(
            functools.partial(attn_kernel, n_col, n_row),
            in_specs=[hbm] * 10,
            out_specs=hbm,
            out_shape=jax.ShapeDtypeStruct((n_col, own, hc, lanes), BF16),
            scratch_shapes=[
                pltpu.VMEM((col_len, chan, row_len), BF16),
                pltpu.VMEM((1, n), res_mask.dtype),
                pltpu.VMEM((1, chan), F32),
                pltpu.VMEM((1, chan), F32),
                pltpu.VMEM(w_q.shape, BF16),
                pltpu.VMEM(w_k.shape, BF16),
                pltpu.VMEM(w_v.shape, BF16),
                pltpu.VMEM(w_g.shape, BF16),
                pltpu.VMEM((heads, chan), BF16),
                pltpu.VMEM(w_o.shape, BF16),
                pltpu.VMEM((heads, col_len, row_len), BF16),
                pltpu.VMEM((row_len, hc, lanes), BF16),
                pltpu.VMEM((n_col, own, hc, lanes), BF16),
                pltpu.VMEM((n_row, heads, n, row_len), BF16),
                pltpu.VMEM((heads, n, n), F32),
                pltpu.VMEM((n, row_len), F32),
                pltpu.VMEM((own, chan, n), F32),
                pltpu.VMEM((own * heads, chan, n), BF16),
                pltpu.VMEM((own, n, chan), BF16),
                pltpu.VMEM((own * heads, hd, n), BF16),
                pltpu.VMEM((own * heads, hd, n), F32),
                pltpu.VMEM((heads, n, n), F32),
                pltpu.VMEM((heads, 1, n), F32),
                pltpu.VMEM((own * heads, hd, n), BF16),
                pltpu.VMEM((n_col, own, hc, lanes), BF16),
                pltpu.VMEM((4 * chan, chan), BF16),
                pltpu.VMEM((chan, chan), BF16),
                pltpu.VMEM((2, chan, row_len), F32),
                dma((10,)),
                dma((heads // 2, n_col - 1)), dma((heads // 2, n_col - 1)),
                dma((n_part, n_col - 1)), dma((n_part, n_col - 1)),
                dma((heads // 2, n_row - 1)), dma((heads // 2, n_row - 1)),
                dma((heads // 2, n_row)), dma((heads // 2, n_row)),
                dma((n_col - 1,)), dma((n_col - 1,)), dma,
            ],
            compiler_params=pltpu.CompilerParams(
                collective_id=0, has_side_effects=True, vmem_limit_bytes=56 << 20),
            name='attention',
        )(jnp.transpose(pair_tile, (1, 2, 0)), res_mask.reshape(1, n), ln_gamma.reshape(1, chan),
          ln_beta.reshape(1, chan), w_q, w_k, w_v, w_g, w_b.T, w_o)

        pairs = 16
        out = pl.pallas_call(
            unpack_kernel,
            grid=(hc // pairs,),
            in_specs=[pl.BlockSpec((row_len, pairs, lanes), lambda i: (0, i, 0))],
            out_specs=pl.BlockSpec((col_len, 2, pairs, row_len), lambda i: (0, 0, i, 0)),
            out_shape=jax.ShapeDtypeStruct((col_len, 2, hc, row_len), BF16),
            name='unpack',
        )(res.reshape(row_len, hc, lanes)).reshape(col_len, chan, row_len)
        return jnp.transpose(out, (2, 0, 1))

    return jax.shard_map(per_device, mesh=mesh,
                         in_specs=(tile_spec, P('dp'), P(), P(), P(), P(), P(), P(), P(), P()),
                         out_specs=tile_spec, check_vma=False)
```

```python
import functools

import jax
import jax.numpy as jnp
from jax import lax
from jax.experimental import pallas as pl
from jax.experimental.pallas import tpu as pltpu
from jax.sharding import PartitionSpec as P

LN_EPS = 1e-5
F32 = jnp.float32
BF16 = jnp.bfloat16
MESH = pl.DeviceIdType.MESH

KEYS = 64
TILE = 256


def column(row, lanes):
    return jnp.broadcast_to(row, (lanes, row.shape[-1])).T


def layer_norm(z, gamma, beta, axis):
    mean = jnp.mean(z, axis=axis, keepdims=True)
    cen = z - mean
    var = jnp.mean(cen * cen, axis=axis, keepdims=True)
    return (cen * lax.rsqrt(var + LN_EPS) * gamma + beta).astype(BF16)


def tile_bias(zin, wb_t, gamma, beta, bt):
    n_key, chan, n_q = zin.shape
    heads = bt.shape[0]
    group = 16
    wide = jnp.concatenate([wb_t, wb_t], axis=1)
    wide = jnp.concatenate([wide] * (group // 2), axis=1)
    rows = jnp.concatenate([jnp.broadcast_to(wide[h:h + 1], (group, group * chan)) for h in range(heads)], axis=0)
    own = lax.broadcasted_iota(jnp.int32, rows.shape, 0) % group
    src = lax.broadcasted_iota(jnp.int32, rows.shape, 1) // chan
    big = jnp.where(own == src, rows, 0.0).astype(BF16)

    def body(g, carry):
        start = pl.multiple_of(g * group, group)
        normed = layer_norm(zin[pl.ds(start, group)].astype(F32), gamma[None], beta[None], 1)
        out = jnp.dot(big, normed.reshape(group * chan, n_q), preferred_element_type=F32)
        for h in range(heads):
            bt[h, pl.ds(start, group), :] = out[h * group:(h + 1) * group].astype(BF16)
        return carry

    lax.fori_loop(0, n_key // group, body, 0)


def to_rows(zin, zt):
    n_key, chan, _ = zin.shape
    hc = chan // 2
    for s in range(0, hc, 16):
        a = jnp.swapaxes(zin[:, s:s + 16, :].astype(F32), 0, 1)
        b = jnp.swapaxes(zin[:, hc + s:hc + s + 16, :].astype(F32), 0, 1)
        c = jnp.concatenate([a, b], axis=1)
        c = jnp.stack([c[i].T for i in range(16)], axis=0)
        zt[:, s:s + 16, :] = jnp.swapaxes(c, 0, 1).astype(BF16)


def unpack_kernel(r, out):
    n_key = out.shape[0]
    pairs = r.shape[1]
    c = jnp.swapaxes(r[...].astype(F32), 0, 1)
    c = [c[i].T for i in range(pairs)]
    for half in range(2):
        x = jnp.stack([y[half * n_key:(half + 1) * n_key] for y in c], axis=0)
        out[:, half] = jnp.swapaxes(x, 0, 1).astype(BF16)


def project(r, zbuf, w_t, gamma, beta, heads, zr, qz, kr, vr, gr):
    n_src, _, hc, lanes = zbuf.shape
    chan = 2 * hc
    half = lanes // 2
    n = n_src * half
    hd = chan // heads
    low = lax.broadcasted_iota(jnp.int32, (hc, lanes), 1) < half
    cols = []
    for x in range(n_src // 2):
        a = zbuf[2 * x, r].astype(F32)
        b = zbuf[2 * x + 1, r].astype(F32)
        top = jnp.where(low, a, pltpu.roll(b, half, 1))
        bot = jnp.where(low, pltpu.roll(a, half, 1), b)
        cols.append(jnp.concatenate([top, bot], axis=0))
    z = jnp.concatenate(cols, axis=1)
    zr[r] = z
    proj = jnp.dot(w_t, layer_norm(z, gamma, beta, 0), preferred_element_type=F32)
    q_t = (proj[:chan] * hd ** -0.5).astype(BF16)
    for h in range(heads):
        parts = []
        if h > 0:
            parts.append(jnp.zeros((h * hd, n), BF16))
        parts.append(q_t[h * hd:(h + 1) * hd])
        if h < heads - 1:
            parts.append(jnp.zeros(((heads - 1 - h) * hd, n), BF16))
        qz[r * heads + h] = jnp.concatenate(parts, axis=0)
        vr[r * heads + h] = proj[2 * chan + h * hd:2 * chan + (h + 1) * hd].astype(BF16)
        gr[r * heads + h] = jax.nn.sigmoid(proj[3 * chan + h * hd:3 * chan + (h + 1) * hd])
    kr[r] = proj[chan:2 * chan].T.astype(BF16)


class Logits:
    def __init__(self, slot, row, head, heads, bias, qz, kr, sref, mref):
        self.slot, self.head, self.bias, self.sref, self.mref = slot, head, bias, sref, mref
        self.value = jnp.dot(kr[row], qz[row * heads + head], preferred_element_type=F32)
        self.top = None
        self.done = 0

    def advance(self):
        n = self.sref.shape[-1]
        if self.done == n:
            return
        sl = slice(self.done, self.done + KEYS)
        self.done += KEYS
        part = self.value[sl] + self.bias[self.head, sl, :]
        self.sref[self.slot, sl, :] = part
        top = jnp.max(part.reshape(KEYS // 8, 8, n), axis=0)
        self.top = top if self.top is None else jnp.maximum(self.top, top)

    def end(self):
        while self.done < self.sref.shape[-1]:
            self.advance()
        self.mref[self.slot] = jnp.max(self.top, axis=0, keepdims=True)


def step(s, own, heads, bias, qz, kr, vr, gr, sref, mref, gat, do_ex=True):
    n = sref.shape[-1]
    nxt = s + 1 if isinstance(s, int) else jnp.minimum(s + 1, own - 1)
    pending = None
    for i in range(heads):
        logits = Logits(i, nxt, i, heads, bias, qz, kr, sref, mref)
        if do_ex:
            idx = s * heads + i
            v = vr[idx]
            g = gr[idx]
            outs = []
            for q0 in range(0, n, TILE):
                qs = slice(q0, q0 + TILE)
                peak = jnp.broadcast_to(mref[i, :, qs], (8, TILE))[None]
                total = jnp.zeros((8, TILE), F32)
                acc = None
                for k0 in range(0, n, TILE):
                    parts = []
                    for k1 in range(k0, k0 + TILE, KEYS):
                        p = jnp.exp(sref[i, k1:k1 + KEYS, qs].reshape(KEYS // 8, 8, TILE) - peak)
                        total = total + jnp.sum(p, axis=0)
                        parts.append(p.reshape(KEYS, TILE).astype(BF16))
                        if pending is not None:
                            pending.advance()
                    d = jnp.dot(v[:, k0:k0 + TILE], jnp.concatenate(parts, axis=0), preferred_element_type=F32)
                    acc = d if acc is None else acc + d
                outs.append((g[:, qs] * (acc / jnp.sum(total, axis=0, keepdims=True))).astype(BF16))
            gat[idx] = jnp.concatenate(outs, axis=1)
        if pending is not None:
            pending.end()
        pending = logits
    pending.end()


def finish(r, zr, gat, wo_t, heads, obuf):
    n_src, _, hc, lanes = obuf.shape
    half = lanes // 2
    low = lax.broadcasted_iota(jnp.int32, (hc, lanes), 1) < half
    gated = jnp.concatenate([gat[r * heads + h] for h in range(heads)], axis=0)
    o = zr[r] + jnp.dot(wo_t, gated, preferred_element_type=F32)
    for x in range(n_src // 2):
        top = o[:hc, x * lanes:(x + 1) * lanes]
        bot = o[hc:, x * lanes:(x + 1) * lanes]
        obuf[2 * x, r] = jnp.where(low, top, pltpu.roll(bot, half, 1)).astype(BF16)
        obuf[2 * x + 1, r] = jnp.where(low, pltpu.roll(top, half, 1), bot).astype(BF16)


def attn_kernel(n_col, n_row, zin_h, mask_h, gamma_h, beta_h, wq_h, wk_h, wv_h, wg_h, wb_h, wo_h, res,
                zin, mask, gamma_row, beta_row, w_q, w_k, w_v, w_g, wb_t, w_o,
                bt, zt, zbuf, ball, bias, kb, zr, qz, kr, vr, gr, sref, mref, gat, obuf, w_t, wo_t, affine,
                in_sem, b1_send, b1_recv, z_send, z_recv, b2_send, b2_recv, b3_send, b3_recv,
                o_send, o_recv, own_sem):
    col = lax.axis_index('col')
    row = lax.axis_index('row')
    core = lax.rem(col, 2)
    mate = col + 1 - 2 * core
    heads, cols, strip = bt.shape
    hh = heads // 2
    own = zbuf.shape[1]
    n = sref.shape[-1]
    n_part = z_send.shape[0]
    part = own // n_part

    def at_col(d):
        return lax.rem(col + d, n_col)

    def at_row(d):
        return lax.rem(row + d, n_row)

    def remote(src, dst, send, recv, where):
        return pltpu.make_async_remote_copy(src_ref=src, dst_ref=dst, send_sem=send, recv_sem=recv,
                                            device_id=where, device_id_type=MESH)

    loads = [pltpu.make_async_copy(src, dst, in_sem.at[i]) for i, (src, dst) in enumerate((
        (gamma_h, gamma_row), (beta_h, beta_row), (wb_h, wb_t), (zin_h, zin), (mask_h, mask),
        (wq_h, w_q), (wk_h, w_k), (wv_h, w_v), (wg_h, w_g), (wo_h, w_o)))]
    for c in loads:
        c.start()

    barrier = pltpu.get_barrier_semaphore()
    for d in range(1, n_col):
        pl.semaphore_signal(barrier, inc=1, device_id={'col': at_col(d)}, device_id_type=MESH)
    for d in range(1, n_row):
        pl.semaphore_signal(barrier, inc=1, device_id={'row': at_row(d)}, device_id_type=MESH)

    for c in loads[:4]:
        c.wait()
    ga = column(gamma_row[...], strip)
    be = column(beta_row[...], strip)
    tile_bias(zin, wb_t[...].astype(F32), ga, be, bt)
    pl.semaphore_wait(barrier, n_col + n_row - 2)

    def keys_of(c):
        return pl.ds(pl.multiple_of(c * cols, cols), cols)

    def first(e, d):
        peer = at_col(d)
        head = lax.rem(peer, 2) * hh + e
        return remote(bt.at[head], ball.at[row, head, keys_of(col), :],
                      b1_send.at[e, d - 1], b1_recv.at[e, d - 1], {'col': peer})

    def second(e, src, c, d):
        head = core * hh + e
        return remote(src, ball.at[row, head, keys_of(c), :],
                      b2_send.at[e, d - 1], b2_recv.at[e, d - 1], {'row': at_row(d)})

    near = (1, n_row - 1)
    for e in range(hh):
        for d in range(1, n_col):
            first(e, d).start()
    for e in range(hh):
        for d in near:
            second(e, bt.at[core * hh + e], col, d).start()

    def rows_out(q, d):
        peer = at_col(d)
        return remote(zt.at[pl.ds(peer * own + q * part, part)], zbuf.at[col, pl.ds(q * part, part)],
                      z_send.at[q, d - 1], z_recv.at[q, d - 1], {'col': peer})

    to_rows(zin, zt)
    for q in range(n_part):
        for d in range(1, n_col):
            rows_out(q, d).start()

    for c in loads[4:]:
        c.wait()
    kb[...] = column(jnp.where(mask[...] > 0, 0.0, -1e9).astype(F32), strip)
    w_t[...] = jnp.concatenate([w[...].astype(F32).T for w in (w_q, w_k, w_v, w_g)], axis=0).astype(BF16)
    wo_t[...] = w_o[...].astype(F32).T.astype(BF16)
    affine[0] = ga
    affine[1] = be
    zbuf[col] = zt[pl.ds(col * own, own)]
    for e in range(hh):
        ball[row, core * hh + e, keys_of(col), :] = bt[core * hh + e]
    for d in range(1, n_col):
        src = lax.rem(col + n_col - d, n_col)
        for e in range(hh):
            first(e, d).wait_recv()
            for f in near:
                second(e, ball.at[row, core * hh + e, keys_of(src), :], src, f).start()

    def third(e, d):
        head = core * hh + e
        from_row = lax.rem(row + n_row - d, n_row)
        return remote(ball.at[from_row, head], ball.at[from_row, head],
                      b3_send.at[e, d], b3_recv.at[e, d], {'col': mate})

    def whole_second(e, d):
        head = core * hh + e
        return remote(ball.at[row, head], ball.at[row, head],
                      b2_send.at[e, d - 1], b2_recv.at[e, d - 1], {'row': at_row(d)})

    def beyond(e):
        d = near[e]
        from_row = lax.rem(row + n_row - d, n_row)
        head = core * hh + e
        return remote(ball.at[from_row, head], ball.at[from_row, head],
                      b2_send.at[e, 1], b2_recv.at[e, 1], {'row': at_row(d)})

    def widen(h, d):
        r = lax.rem(row + n_row - d, n_row)
        lanes = pl.ds(pl.multiple_of(r * strip, strip), strip)
        bias[h, :, lanes] = ball[r, h].astype(F32) + kb[...]

    def arrived(e, d):
        whole_second(e, d).wait_recv()
        third(e, d).start()
        widen(core * hh + e, d)

    def take_rows(q):
        for d in range(1, n_col):
            rows_out(q, d).wait_recv()
        wide = [jnp.concatenate([affine[i]] * (n // strip), axis=1) for i in range(2)]

        def body(r, carry):
            project(r, zbuf, w_t[...], wide[0], wide[1], heads, zr, qz, kr, vr, gr)
            return carry

        lax.fori_loop(q * part, (q + 1) * part, body, 0)

    run = functools.partial(step, own=own, heads=heads, bias=bias, qz=qz, kr=kr, vr=vr,
                            gr=gr, sref=sref, mref=mref, gat=gat)

    def make_row(r):
        finish(r, zr, gat, wo_t[...], heads, obuf)

    def give_row(r):
        for d in range(1, n_col):
            peer = at_col(d)
            remote(obuf.at[peer, r], res.at[col, r], o_send.at[d - 1], o_recv.at[d - 1], {'col': peer}).start()

    for e in range(hh):
        third(e, 0).start()
        widen(core * hh + e, 0)
    for e in range(hh):
        whole_second(e, near[e]).wait_recv()
        beyond(e).start()
        third(e, near[e]).start()
    take_rows(0)
    for e in range(hh):
        widen(core * hh + e, near[e])
        arrived(e, near[1 - e])
    take_rows(1)
    take_rows(2)
    for e in range(hh):
        arrived(e, 2)
    take_rows(3)
    for d in (0, 1, n_row - 1, 2):
        for e in range(hh):
            third(e, d).wait_recv()
            widen((1 - core) * hh + e, d)

    run(-1, do_ex=False)
    run(0)

    def body(s, carry):
        make_row(s - 1)
        run(s)
        give_row(s - 1)
        return carry

    lax.fori_loop(1, own, body, 0)
    make_row(own - 1)
    give_row(own - 1)

    mine = pltpu.make_async_copy(obuf.at[col], res.at[col], own_sem)
    mine.start()
    for e in range(hh):
        for d in range(1, n_col):
            first(e, d).wait_send()
        for d in near:
            whole_second(e, d).wait_send()
        beyond(e).wait_send()
        for d in range(n_row):
            third(e, d).wait_send()
    for q in range(n_part):
        for d in range(1, n_col):
            rows_out(q, d).wait_send()
    for d in range(1, n_col):
        peer = at_col(d)
        whole = remote(obuf.at[peer], res.at[col], o_send.at[d - 1], o_recv.at[d - 1], {'col': peer})
        whole.wait_send()
        whole.wait_recv()
    mine.wait()


def solution(mesh):
    n_col = mesh.shape['col']
    n_row = mesh.shape['row']
    tile_spec = P(('dp', 'row'), 'col', None)
    hbm = pl.BlockSpec(memory_space=pltpu.HBM)
    n_part = 4

    def per_device(pair_tile, res_mask, ln_gamma, ln_beta, w_q, w_k, w_v, w_b, w_g, w_o):
        row_len, col_len, chan = pair_tile.shape
        heads = w_b.shape[1]
        hd = chan // heads
        n = res_mask.shape[0]
        own = row_len // n_col
        hc = chan // 2
        lanes = 2 * col_len
        dma = pltpu.SemaphoreType.DMA
        res = pl.pallas_call(
            functools.partial(attn_kernel, n_col, n_row),
            in_specs=[hbm] * 10,
            out_specs=hbm,
            out_shape=jax.ShapeDtypeStruct((n_col, own, hc, lanes), BF16),
            scratch_shapes=[
                pltpu.VMEM((col_len, chan, row_len), BF16),
                pltpu.VMEM((1, n), res_mask.dtype),
                pltpu.VMEM((1, chan), F32),
                pltpu.VMEM((1, chan), F32),
                pltpu.VMEM(w_q.shape, BF16),
                pltpu.VMEM(w_k.shape, BF16),
                pltpu.VMEM(w_v.shape, BF16),
                pltpu.VMEM(w_g.shape, BF16),
                pltpu.VMEM((heads, chan), BF16),
                pltpu.VMEM(w_o.shape, BF16),
                pltpu.VMEM((heads, col_len, row_len), BF16),
                pltpu.VMEM((row_len, hc, lanes), BF16),
                pltpu.VMEM((n_col, own, hc, lanes), BF16),
                pltpu.VMEM((n_row, heads, n, row_len), BF16),
                pltpu.VMEM((heads, n, n), F32),
                pltpu.VMEM((n, row_len), F32),
                pltpu.VMEM((own, chan, n), F32),
                pltpu.VMEM((own * heads, chan, n), BF16),
                pltpu.VMEM((own, n, chan), BF16),
                pltpu.VMEM((own * heads, hd, n), BF16),
                pltpu.VMEM((own * heads, hd, n), F32),
                pltpu.VMEM((heads, n, n), F32),
                pltpu.VMEM((heads, 1, n), F32),
                pltpu.VMEM((own * heads, hd, n), BF16),
                pltpu.VMEM((n_col, own, hc, lanes), BF16),
                pltpu.VMEM((4 * chan, chan), BF16),
                pltpu.VMEM((chan, chan), BF16),
                pltpu.VMEM((2, chan, row_len), F32),
                dma((10,)),
                dma((heads // 2, n_col - 1)), dma((heads // 2, n_col - 1)),
                dma((n_part, n_col - 1)), dma((n_part, n_col - 1)),
                dma((heads // 2, n_row - 1)), dma((heads // 2, n_row - 1)),
                dma((heads // 2, n_row)), dma((heads // 2, n_row)),
                dma((n_col - 1,)), dma((n_col - 1,)), dma,
            ],
            compiler_params=pltpu.CompilerParams(
                collective_id=0, has_side_effects=True, vmem_limit_bytes=56 << 20),
            name='attention',
        )(jnp.transpose(pair_tile, (1, 2, 0)), res_mask.reshape(1, n), ln_gamma.reshape(1, chan),
          ln_beta.reshape(1, chan), w_q, w_k, w_v, w_g, w_b.T, w_o)

        pairs = 16
        out = pl.pallas_call(
            unpack_kernel,
            grid=(hc // pairs,),
            in_specs=[pl.BlockSpec((row_len, pairs, lanes), lambda i: (0, i, 0))],
            out_specs=pl.BlockSpec((col_len, 2, pairs, row_len), lambda i: (0, 0, i, 0)),
            out_shape=jax.ShapeDtypeStruct((col_len, 2, hc, row_len), BF16),
            name='unpack',
        )(res.reshape(row_len, hc, lanes)).reshape(col_len, chan, row_len)
        return jnp.transpose(out, (2, 0, 1))

    return jax.shard_map(per_device, mesh=mesh,
                         in_specs=(tile_spec, P('dp'), P(), P(), P(), P(), P(), P(), P(), P()),
                         out_specs=tile_spec, check_vma=False)
```

```python
import functools

import jax
import jax.numpy as jnp
from jax import lax
from jax.experimental import pallas as pl
from jax.experimental.pallas import tpu as pltpu
from jax.sharding import PartitionSpec as P

LN_EPS = 1e-5
F32 = jnp.float32
BF16 = jnp.bfloat16
MESH = pl.DeviceIdType.MESH

KEYS = 64
TILE = 256


def column(row, lanes):
    return jnp.broadcast_to(row, (lanes, row.shape[-1])).T


def layer_norm(z, gamma, beta, axis):
    mean = jnp.mean(z, axis=axis, keepdims=True)
    cen = z - mean
    var = jnp.mean(cen * cen, axis=axis, keepdims=True)
    return (cen * lax.rsqrt(var + LN_EPS) * gamma + beta).astype(BF16)


def tile_bias(zin, wb_t, gamma, beta, bt):
    n_key, chan, n_q = zin.shape
    heads = bt.shape[0]
    group = 16
    wide = jnp.concatenate([wb_t, wb_t], axis=1)
    wide = jnp.concatenate([wide] * (group // 2), axis=1)
    rows = jnp.concatenate([jnp.broadcast_to(wide[h:h + 1], (group, group * chan)) for h in range(heads)], axis=0)
    own = lax.broadcasted_iota(jnp.int32, rows.shape, 0) % group
    src = lax.broadcasted_iota(jnp.int32, rows.shape, 1) // chan
    big = jnp.where(own == src, rows, 0.0).astype(BF16)

    def body(g, carry):
        start = pl.multiple_of(g * group, group)
        normed = layer_norm(zin[pl.ds(start, group)].astype(F32), gamma[None], beta[None], 1)
        out = jnp.dot(big, normed.reshape(group * chan, n_q), preferred_element_type=F32)
        for h in range(heads):
            bt[h, pl.ds(start, group), :] = out[h * group:(h + 1) * group].astype(BF16)
        return carry

    lax.fori_loop(0, n_key // group, body, 0)


def to_rows(zin, zt):
    n_key, chan, _ = zin.shape
    hc = chan // 2
    for s in range(0, hc, 16):
        a = jnp.swapaxes(zin[:, s:s + 16, :].astype(F32), 0, 1)
        b = jnp.swapaxes(zin[:, hc + s:hc + s + 16, :].astype(F32), 0, 1)
        c = jnp.concatenate([a, b], axis=1)
        c = jnp.stack([c[i].T for i in range(16)], axis=0)
        zt[:, s:s + 16, :] = jnp.swapaxes(c, 0, 1).astype(BF16)


def unpack_kernel(r, out):
    n_key = out.shape[0]
    pairs = r.shape[1]
    c = jnp.swapaxes(r[...].astype(F32), 0, 1)
    c = [c[i].T for i in range(pairs)]
    for half in range(2):
        x = jnp.stack([y[half * n_key:(half + 1) * n_key] for y in c], axis=0)
        out[:, half] = jnp.swapaxes(x, 0, 1).astype(BF16)


def project(r, zbuf, w_t, gamma, beta, heads, zr, qz, kr, vr, gr):
    n_src, _, hc, lanes = zbuf.shape
    chan = 2 * hc
    half = lanes // 2
    n = n_src * half
    hd = chan // heads
    low = lax.broadcasted_iota(jnp.int32, (hc, lanes), 1) < half
    cols = []
    for x in range(n_src // 2):
        a = zbuf[2 * x, r].astype(F32)
        b = zbuf[2 * x + 1, r].astype(F32)
        top = jnp.where(low, a, pltpu.roll(b, half, 1))
        bot = jnp.where(low, pltpu.roll(a, half, 1), b)
        cols.append(jnp.concatenate([top, bot], axis=0))
    z = jnp.concatenate(cols, axis=1)
    zr[r] = z
    proj = jnp.dot(w_t, layer_norm(z, gamma, beta, 0), preferred_element_type=F32)
    q_t = (proj[:chan] * hd ** -0.5).astype(BF16)
    for h in range(heads):
        parts = []
        if h > 0:
            parts.append(jnp.zeros((h * hd, n), BF16))
        parts.append(q_t[h * hd:(h + 1) * hd])
        if h < heads - 1:
            parts.append(jnp.zeros(((heads - 1 - h) * hd, n), BF16))
        qz[r * heads + h] = jnp.concatenate(parts, axis=0)
        vr[r * heads + h] = proj[2 * chan + h * hd:2 * chan + (h + 1) * hd].astype(BF16)
        gr[r * heads + h] = jax.nn.sigmoid(proj[3 * chan + h * hd:3 * chan + (h + 1) * hd])
    kr[r] = proj[chan:2 * chan].T.astype(BF16)


class Logits:
    def __init__(self, slot, row, head, heads, bias, qz, kr, sref, mref):
        self.slot, self.head, self.bias, self.sref, self.mref = slot, head, bias, sref, mref
        self.value = jnp.dot(kr[row], qz[row * heads + head], preferred_element_type=F32)
        self.top = None
        self.done = 0

    def advance(self):
        n = self.sref.shape[-1]
        if self.done == n:
            return
        sl = slice(self.done, self.done + KEYS)
        self.done += KEYS
        part = self.value[sl] + self.bias[self.head, sl, :]
        self.sref[self.slot, sl, :] = part
        top = jnp.max(part.reshape(KEYS // 8, 8, n), axis=0)
        self.top = top if self.top is None else jnp.maximum(self.top, top)

    def end(self):
        while self.done < self.sref.shape[-1]:
            self.advance()
        self.mref[self.slot] = jnp.max(self.top, axis=0, keepdims=True)


def step(s, own, heads, bias, qz, kr, vr, gr, sref, mref, gat, do_ex=True):
    n = sref.shape[-1]
    nxt = s + 1 if isinstance(s, int) else jnp.minimum(s + 1, own - 1)
    pending = None
    for i in range(heads):
        logits = Logits(i, nxt, i, heads, bias, qz, kr, sref, mref)
        if do_ex:
            idx = s * heads + i
            v = vr[idx]
            g = gr[idx]
            outs = []
            for q0 in range(0, n, TILE):
                qs = slice(q0, q0 + TILE)
                peak = jnp.broadcast_to(mref[i, :, qs], (8, TILE))[None]
                total = jnp.zeros((8, TILE), F32)
                acc = None
                for k0 in range(0, n, TILE):
                    parts = []
                    for k1 in range(k0, k0 + TILE, KEYS):
                        p = jnp.exp(sref[i, k1:k1 + KEYS, qs].reshape(KEYS // 8, 8, TILE) - peak)
                        total = total + jnp.sum(p, axis=0)
                        parts.append(p.reshape(KEYS, TILE).astype(BF16))
                        if pending is not None:
                            pending.advance()
                    d = jnp.dot(v[:, k0:k0 + TILE], jnp.concatenate(parts, axis=0), preferred_element_type=F32)
                    acc = d if acc is None else acc + d
                outs.append((g[:, qs] * (acc / jnp.sum(total, axis=0, keepdims=True))).astype(BF16))
            gat[idx] = jnp.concatenate(outs, axis=1)
        if pending is not None:
            pending.end()
        pending = logits
    pending.end()


def finish(r, zr, gat, wo_t, heads, obuf):
    n_src, _, hc, lanes = obuf.shape
    half = lanes // 2
    low = lax.broadcasted_iota(jnp.int32, (hc, lanes), 1) < half
    gated = jnp.concatenate([gat[r * heads + h] for h in range(heads)], axis=0)
    o = zr[r] + jnp.dot(wo_t, gated, preferred_element_type=F32)
    for x in range(n_src // 2):
        top = o[:hc, x * lanes:(x + 1) * lanes]
        bot = o[hc:, x * lanes:(x + 1) * lanes]
        obuf[2 * x, r] = jnp.where(low, top, pltpu.roll(bot, half, 1)).astype(BF16)
        obuf[2 * x + 1, r] = jnp.where(low, pltpu.roll(top, half, 1), bot).astype(BF16)


def attn_kernel(n_col, n_row, zin_h, mask_h, gamma_h, beta_h, wq_h, wk_h, wv_h, wg_h, wb_h, wo_h, res,
                zin, mask, gamma_row, beta_row, w_q, w_k, w_v, w_g, wb_t, w_o,
                bt, zt, zbuf, ball, bias, kb, zr, qz, kr, vr, gr, sref, mref, gat, obuf, w_t, wo_t, affine,
                in_sem, b1_send, b1_recv, z_send, z_recv, b2_send, b2_recv, b3_send, b3_recv,
                o_send, o_recv, own_sem):
    col = lax.axis_index('col')
    row = lax.axis_index('row')
    core = lax.rem(col, 2)
    mate = col + 1 - 2 * core
    heads, cols, strip = bt.shape
    hh = heads // 2
    own = zbuf.shape[1]
    n = sref.shape[-1]
    n_part = z_send.shape[0]
    part = own // n_part

    def at_col(d):
        return lax.rem(col + d, n_col)

    def at_row(d):
        return lax.rem(row + d, n_row)

    def remote(src, dst, send, recv, where):
        return pltpu.make_async_remote_copy(src_ref=src, dst_ref=dst, send_sem=send, recv_sem=recv,
                                            device_id=where, device_id_type=MESH)

    loads = [pltpu.make_async_copy(src, dst, in_sem.at[i]) for i, (src, dst) in enumerate((
        (gamma_h, gamma_row), (beta_h, beta_row), (wb_h, wb_t), (zin_h, zin), (mask_h, mask),
        (wq_h, w_q), (wk_h, w_k), (wv_h, w_v), (wg_h, w_g), (wo_h, w_o)))]
    for c in loads:
        c.start()

    barrier = pltpu.get_barrier_semaphore()
    for d in range(1, n_col):
        pl.semaphore_signal(barrier, inc=1, device_id={'col': at_col(d)}, device_id_type=MESH)
    for d in range(1, n_row):
        pl.semaphore_signal(barrier, inc=1, device_id={'row': at_row(d)}, device_id_type=MESH)

    for c in loads[:4]:
        c.wait()
    ga = column(gamma_row[...], strip)
    be = column(beta_row[...], strip)
    tile_bias(zin, wb_t[...].astype(F32), ga, be, bt)
    pl.semaphore_wait(barrier, n_col + n_row - 2)

    def keys_of(c):
        return pl.ds(pl.multiple_of(c * cols, cols), cols)

    def first(e, d):
        peer = at_col(d)
        head = lax.rem(peer, 2) * hh + e
        return remote(bt.at[head], ball.at[row, head, keys_of(col), :],
                      b1_send.at[e, d - 1], b1_recv.at[e, d - 1], {'col': peer})

    def second(e, src, c, d):
        head = core * hh + e
        return remote(src, ball.at[row, head, keys_of(c), :],
                      b2_send.at[e, d - 1], b2_recv.at[e, d - 1], {'row': at_row(d)})

    near = (1, n_row - 1)
    for e in range(hh):
        for d in range(1, n_col):
            first(e, d).start()
    for e in range(hh):
        for d in near:
            second(e, bt.at[core * hh + e], col, d).start()

    def rows_out(q, d):
        peer = at_col(d)
        return remote(zt.at[pl.ds(peer * own + q * part, part)], zbuf.at[col, pl.ds(q * part, part)],
                      z_send.at[q, d - 1], z_recv.at[q, d - 1], {'col': peer})

    to_rows(zin, zt)
    for q in range(n_part):
        for d in range(1, n_col):
            rows_out(q, d).start()

    for c in loads[4:]:
        c.wait()
    kb[...] = column(jnp.where(mask[...] > 0, 0.0, -1e9).astype(F32), strip)
    w_t[...] = jnp.concatenate([w[...].astype(F32).T for w in (w_q, w_k, w_v, w_g)], axis=0).astype(BF16)
    wo_t[...] = w_o[...].astype(F32).T.astype(BF16)
    affine[0] = ga
    affine[1] = be
    zbuf[col] = zt[pl.ds(col * own, own)]
    for e in range(hh):
        ball[row, core * hh + e, keys_of(col), :] = bt[core * hh + e]
    for d in range(1, n_col):
        src = lax.rem(col + n_col - d, n_col)
        for e in range(hh):
            first(e, d).wait_recv()
            for f in near:
                second(e, ball.at[row, core * hh + e, keys_of(src), :], src, f).start()

    def third(e, d):
        head = core * hh + e
        from_row = lax.rem(row + n_row - d, n_row)
        return remote(ball.at[from_row, head], ball.at[from_row, head],
                      b3_send.at[e, d], b3_recv.at[e, d], {'col': mate})

    def whole_second(e, d):
        head = core * hh + e
        return remote(ball.at[row, head], ball.at[row, head],
                      b2_send.at[e, d - 1], b2_recv.at[e, d - 1], {'row': at_row(d)})

    def beyond(e):
        d = near[e]
        from_row = lax.rem(row + n_row - d, n_row)
        head = core * hh + e
        return remote(ball.at[from_row, head], ball.at[from_row, head],
                      b2_send.at[e, 1], b2_recv.at[e, 1], {'row': at_row(d)})

    def widen(h, d):
        r = lax.rem(row + n_row - d, n_row)
        lanes = pl.ds(pl.multiple_of(r * strip, strip), strip)
        bias[h, :, lanes] = ball[r, h].astype(F32) + kb[...]

    def arrived(e, d):
        whole_second(e, d).wait_recv()
        third(e, d).start()
        widen(core * hh + e, d)

    def take_rows(q):
        for d in range(1, n_col):
            rows_out(q, d).wait_recv()
        wide = [jnp.concatenate([affine[i]] * (n // strip), axis=1) for i in range(2)]

        def body(r, carry):
            project(r, zbuf, w_t[...], wide[0], wide[1], heads, zr, qz, kr, vr, gr)
            return carry

        lax.fori_loop(q * part, (q + 1) * part, body, 0)

    run = functools.partial(step, own=own, heads=heads, bias=bias, qz=qz, kr=kr, vr=vr,
                            gr=gr, sref=sref, mref=mref, gat=gat)

    def make_row(r):
        finish(r, zr, gat, wo_t[...], heads, obuf)

    def give_row(r):
        for d in range(1, n_col):
            peer = at_col(d)
            remote(obuf.at[peer, r], res.at[col, r], o_send.at[d - 1], o_recv.at[d - 1], {'col': peer}).start()

    for e in range(hh):
        third(e, 0).start()
        widen(core * hh + e, 0)
    for e in range(hh):
        whole_second(e, near[e]).wait_recv()
        beyond(e).start()
        third(e, near[e]).start()
    take_rows(0)
    for e in range(hh):
        widen(core * hh + e, near[e])
        arrived(e, near[1 - e])
    take_rows(1)
    for e in range(hh):
        arrived(e, 2)
    for d in (0, 1, n_row - 1, 2):
        for e in range(hh):
            third(e, d).wait_recv()
            widen((1 - core) * hh + e, d)

    run(-1, do_ex=False)
    run(0)

    def body(s, carry):
        for q in range(2, n_part):
            pl.when(s == q * part - 3)(functools.partial(take_rows, q))

        make_row(s - 1)
        run(s)
        give_row(s - 1)
        return carry

    lax.fori_loop(1, own, body, 0)
    make_row(own - 1)
    give_row(own - 1)

    mine = pltpu.make_async_copy(obuf.at[col], res.at[col], own_sem)
    mine.start()
    for e in range(hh):
        for d in range(1, n_col):
            first(e, d).wait_send()
        for d in near:
            whole_second(e, d).wait_send()
        beyond(e).wait_send()
        for d in range(n_row):
            third(e, d).wait_send()
    for q in range(n_part):
        for d in range(1, n_col):
            rows_out(q, d).wait_send()
    for d in range(1, n_col):
        peer = at_col(d)
        whole = remote(obuf.at[peer], res.at[col], o_send.at[d - 1], o_recv.at[d - 1], {'col': peer})
        whole.wait_send()
        whole.wait_recv()
    mine.wait()


def solution(mesh):
    n_col = mesh.shape['col']
    n_row = mesh.shape['row']
    tile_spec = P(('dp', 'row'), 'col', None)
    hbm = pl.BlockSpec(memory_space=pltpu.HBM)
    n_part = 4

    def per_device(pair_tile, res_mask, ln_gamma, ln_beta, w_q, w_k, w_v, w_b, w_g, w_o):
        row_len, col_len, chan = pair_tile.shape
        heads = w_b.shape[1]
        hd = chan // heads
        n = res_mask.shape[0]
        own = row_len // n_col
        hc = chan // 2
        lanes = 2 * col_len
        dma = pltpu.SemaphoreType.DMA
        res = pl.pallas_call(
            functools.partial(attn_kernel, n_col, n_row),
            in_specs=[hbm] * 10,
            out_specs=hbm,
            out_shape=jax.ShapeDtypeStruct((n_col, own, hc, lanes), BF16),
            scratch_shapes=[
                pltpu.VMEM((col_len, chan, row_len), BF16),
                pltpu.VMEM((1, n), res_mask.dtype),
                pltpu.VMEM((1, chan), F32),
                pltpu.VMEM((1, chan), F32),
                pltpu.VMEM(w_q.shape, BF16),
                pltpu.VMEM(w_k.shape, BF16),
                pltpu.VMEM(w_v.shape, BF16),
                pltpu.VMEM(w_g.shape, BF16),
                pltpu.VMEM((heads, chan), BF16),
                pltpu.VMEM(w_o.shape, BF16),
                pltpu.VMEM((heads, col_len, row_len), BF16),
                pltpu.VMEM((row_len, hc, lanes), BF16),
                pltpu.VMEM((n_col, own, hc, lanes), BF16),
                pltpu.VMEM((n_row, heads, n, row_len), BF16),
                pltpu.VMEM((heads, n, n), F32),
                pltpu.VMEM((n, row_len), F32),
                pltpu.VMEM((own, chan, n), F32),
                pltpu.VMEM((own * heads, chan, n), BF16),
                pltpu.VMEM((own, n, chan), BF16),
                pltpu.VMEM((own * heads, hd, n), BF16),
                pltpu.VMEM((own * heads, hd, n), F32),
                pltpu.VMEM((heads, n, n), F32),
                pltpu.VMEM((heads, 1, n), F32),
                pltpu.VMEM((own * heads, hd, n), BF16),
                pltpu.VMEM((n_col, own, hc, lanes), BF16),
                pltpu.VMEM((4 * chan, chan), BF16),
                pltpu.VMEM((chan, chan), BF16),
                pltpu.VMEM((2, chan, row_len), F32),
                dma((10,)),
                dma((heads // 2, n_col - 1)), dma((heads // 2, n_col - 1)),
                dma((n_part, n_col - 1)), dma((n_part, n_col - 1)),
                dma((heads // 2, n_row - 1)), dma((heads // 2, n_row - 1)),
                dma((heads // 2, n_row)), dma((heads // 2, n_row)),
                dma((n_col - 1,)), dma((n_col - 1,)), dma,
            ],
            compiler_params=pltpu.CompilerParams(
                collective_id=0, has_side_effects=True, vmem_limit_bytes=56 << 20),
            name='attention',
        )(jnp.transpose(pair_tile, (1, 2, 0)), res_mask.reshape(1, n), ln_gamma.reshape(1, chan),
          ln_beta.reshape(1, chan), w_q, w_k, w_v, w_g, w_b.T, w_o)

        pairs = 16
        out = pl.pallas_call(
            unpack_kernel,
            grid=(hc // pairs,),
            in_specs=[pl.BlockSpec((row_len, pairs, lanes), lambda i: (0, i, 0))],
            out_specs=pl.BlockSpec((col_len, 2, pairs, row_len), lambda i: (0, 0, i, 0)),
            out_shape=jax.ShapeDtypeStruct((col_len, 2, hc, row_len), BF16),
            name='unpack',
        )(res.reshape(row_len, hc, lanes)).reshape(col_len, chan, row_len)
        return jnp.transpose(out, (2, 0, 1))

    return jax.shard_map(per_device, mesh=mesh,
                         in_specs=(tile_spec, P('dp'), P(), P(), P(), P(), P(), P(), P(), P()),
                         out_specs=tile_spec, check_vma=False)
```

```python
import functools

import jax
import jax.numpy as jnp
from jax import lax
from jax.experimental import pallas as pl
from jax.experimental.pallas import tpu as pltpu
from jax.sharding import PartitionSpec as P

LN_EPS = 1e-5
F32 = jnp.float32
BF16 = jnp.bfloat16
MESH = pl.DeviceIdType.MESH

KEYS = 64
TILE = 256


def column(row, lanes):
    return jnp.broadcast_to(row, (lanes, row.shape[-1])).T


def layer_norm(z, gamma, beta, axis):
    mean = jnp.mean(z, axis=axis, keepdims=True)
    cen = z - mean
    var = jnp.mean(cen * cen, axis=axis, keepdims=True)
    return (cen * lax.rsqrt(var + LN_EPS) * gamma + beta).astype(BF16)


def tile_bias(zin, wb_t, gamma, beta, bt):
    n_key, chan, n_q = zin.shape
    heads = bt.shape[0]
    group = 16
    wide = jnp.concatenate([wb_t, wb_t], axis=1)
    wide = jnp.concatenate([wide] * (group // 2), axis=1)
    rows = jnp.concatenate([jnp.broadcast_to(wide[h:h + 1], (group, group * chan)) for h in range(heads)], axis=0)
    own = lax.broadcasted_iota(jnp.int32, rows.shape, 0) % group
    src = lax.broadcasted_iota(jnp.int32, rows.shape, 1) // chan
    big = jnp.where(own == src, rows, 0.0).astype(BF16)

    def body(g, carry):
        start = pl.multiple_of(g * group, group)
        normed = layer_norm(zin[pl.ds(start, group)].astype(F32), gamma[None], beta[None], 1)
        out = jnp.dot(big, normed.reshape(group * chan, n_q), preferred_element_type=F32)
        for h in range(heads):
            bt[h, pl.ds(start, group), :] = out[h * group:(h + 1) * group].astype(BF16)
        return carry

    lax.fori_loop(0, n_key // group, body, 0)


def to_rows(zin, zt):
    n_key, chan, _ = zin.shape
    hc = chan // 2
    for s in range(0, hc, 16):
        a = jnp.swapaxes(zin[:, s:s + 16, :].astype(F32), 0, 1)
        b = jnp.swapaxes(zin[:, hc + s:hc + s + 16, :].astype(F32), 0, 1)
        c = jnp.concatenate([a, b], axis=1)
        c = jnp.stack([c[i].T for i in range(16)], axis=0)
        zt[:, s:s + 16, :] = jnp.swapaxes(c, 0, 1).astype(BF16)


def unpack_kernel(r, out):
    n_key = out.shape[0]
    pairs = r.shape[1]
    c = jnp.swapaxes(r[...].astype(F32), 0, 1)
    c = [c[i].T for i in range(pairs)]
    for half in range(2):
        x = jnp.stack([y[half * n_key:(half + 1) * n_key] for y in c], axis=0)
        out[:, half] = jnp.swapaxes(x, 0, 1).astype(BF16)


def strip_at(row, n_row, pos):
    return lax.rem(row + n_row - (0, 1, n_row - 1, 2)[pos], n_row)


def place_of(row, n_row, strip):
    back = lax.rem(row + n_row - strip, n_row)
    return jnp.where(back < 2, back, n_row + 1 - back)


def project(r, place, zbuf, w_t, gamma, beta, heads, zr, qz, kr, vr, gr):
    n_src, _, hc, lanes = zbuf.shape
    chan = 2 * hc
    half = lanes // 2
    n = n_src * half
    hd = chan // heads
    low = lax.broadcasted_iota(jnp.int32, (hc, lanes), 1) < half
    cols = []
    for x in range(n_src // 2):
        a = zbuf[2 * x, r].astype(F32)
        b = zbuf[2 * x + 1, r].astype(F32)
        top = jnp.where(low, a, pltpu.roll(b, half, 1))
        bot = jnp.where(low, pltpu.roll(a, half, 1), b)
        cols.append(jnp.concatenate([top, bot], axis=0))
    z = jnp.concatenate(cols, axis=1)
    proj = jnp.dot(w_t, layer_norm(z, gamma, beta, 0), preferred_element_type=F32)
    q_t = (proj[:chan] * hd ** -0.5).astype(BF16)
    gates = jax.nn.sigmoid(proj[3 * chan:])
    strip = lanes
    for x, pos in enumerate(place):
        cs = slice(x * strip, (x + 1) * strip)
        side = pos // 2
        lane = pl.ds(pl.multiple_of((pos % 2) * strip, strip), strip)
        zr[side, r, :, lane] = z[:, cs]
        for h in range(heads):
            parts = []
            if h > 0:
                parts.append(jnp.zeros((h * hd, strip), BF16))
            parts.append(q_t[h * hd:(h + 1) * hd, cs])
            if h < heads - 1:
                parts.append(jnp.zeros(((heads - 1 - h) * hd, strip), BF16))
            qz[side, r * heads + h, :, lane] = jnp.concatenate(parts, axis=0)
            gr[side, r * heads + h, :, lane] = gates[h * hd:(h + 1) * hd, cs]
    for h in range(heads):
        vr[r * heads + h] = proj[2 * chan + h * hd:2 * chan + (h + 1) * hd].astype(BF16)
    kr[r] = proj[chan:2 * chan].T.astype(BF16)


class Logits:
    def __init__(self, slot, side, row, head, heads, bias, qz, kr, sref, mref):
        self.slot, self.side, self.head, self.bias, self.sref, self.mref = slot, side, head, bias, sref, mref
        self.value = jnp.dot(kr[row], qz[side, row * heads + head], preferred_element_type=F32)
        self.top = None
        self.done = 0

    def advance(self):
        _, n, width = self.sref.shape
        if self.done == n:
            return
        sl = slice(self.done, self.done + KEYS)
        self.done += KEYS
        part = self.value[sl] + self.bias[self.side, self.head, sl, :]
        self.sref[self.slot, sl, :] = part
        top = jnp.max(part.reshape(KEYS // 8, 8, width), axis=0)
        self.top = top if self.top is None else jnp.maximum(self.top, top)

    def end(self):
        while self.done < self.sref.shape[1]:
            self.advance()
        self.mref[self.slot] = jnp.max(self.top, axis=0, keepdims=True)


def where_of(t, early):
    split = t < 2 * early
    pair = jnp.where(split, t % early, early + (t - 2 * early) // 2)
    side = jnp.where(split, t // early, t % 2)
    return pair, side


def step(t, early, n_step, heads, bias, qz, kr, vr, gr, sref, mref, gat, do_ex=True):
    slots, n, width = sref.shape
    nxt = t + 1 if isinstance(t, int) else jnp.minimum(t + 1, n_step - 1)
    n_pair, n_side = where_of(nxt, early)
    pair, side = where_of(t, early)
    pending = None
    for i in range(slots):
        logits = Logits(i, n_side, 2 * n_pair + i // heads, i % heads, heads, bias, qz, kr, sref, mref)
        if do_ex:
            idx = (2 * pair + i // heads) * heads + i % heads
            v = vr[idx]
            peak = jnp.broadcast_to(mref[i], (8, width))[None]
            total = jnp.zeros((8, width), F32)
            acc = None
            for k0 in range(0, n, TILE):
                parts = []
                for k1 in range(k0, k0 + TILE, KEYS):
                    p = jnp.exp(sref[i, k1:k1 + KEYS].reshape(KEYS // 8, 8, width) - peak)
                    total = total + jnp.sum(p, axis=0)
                    parts.append(p.reshape(KEYS, width).astype(BF16))
                    if pending is not None:
                        pending.advance()
                d = jnp.dot(v[:, k0:k0 + TILE], jnp.concatenate(parts, axis=0), preferred_element_type=F32)
                acc = d if acc is None else acc + d
            gat[side, idx] = (gr[side, idx] * (acc / jnp.sum(total, axis=0, keepdims=True))).astype(BF16)
        if pending is not None:
            pending.end()
        pending = logits
    pending.end()


def finish(r, side, chips, zr, gat, wo_t, heads, obuf):
    _, _, hc, lanes = obuf.shape
    half = lanes // 2
    low = lax.broadcasted_iota(jnp.int32, (hc, lanes), 1) < half
    gated = jnp.concatenate([gat[side, r * heads + h] for h in range(heads)], axis=0)
    o = zr[side, r] + jnp.dot(wo_t, gated, preferred_element_type=F32)
    for j, x in enumerate(chips):
        top = o[:hc, j * lanes:(j + 1) * lanes]
        bot = o[hc:, j * lanes:(j + 1) * lanes]
        obuf[2 * x, r] = jnp.where(low, top, pltpu.roll(bot, half, 1)).astype(BF16)
        obuf[2 * x + 1, r] = jnp.where(low, pltpu.roll(top, half, 1), bot).astype(BF16)


def attn_kernel(n_col, n_row, zin_h, mask_h, gamma_h, beta_h, wq_h, wk_h, wv_h, wg_h, wb_h, wo_h, res,
                zin, mask, gamma_row, beta_row, w_q, w_k, w_v, w_g, wb_t, w_o,
                bt, zt, zbuf, ball, bias, kb, zr, qz, kr, vr, gr, sref, mref, gat, obuf, w_t, wo_t, affine,
                in_sem, b1_send, b1_recv, z_send, z_recv, b2_send, b2_recv, b3_send, b3_recv,
                o_send, o_recv, own_sem):
    col = lax.axis_index('col')
    row = lax.axis_index('row')
    core = lax.rem(col, 2)
    mate = col + 1 - 2 * core
    heads, cols, strip = bt.shape
    hh = heads // 2
    own = zbuf.shape[1]
    n = sref.shape[1]
    n_part = z_send.shape[0]
    part = own // n_part
    early = own // 4
    n_step = own

    def at_col(d):
        return lax.rem(col + d, n_col)

    def at_row(d):
        return lax.rem(row + d, n_row)

    def remote(src, dst, send, recv, where):
        return pltpu.make_async_remote_copy(src_ref=src, dst_ref=dst, send_sem=send, recv_sem=recv,
                                            device_id=where, device_id_type=MESH)

    loads = [pltpu.make_async_copy(src, dst, in_sem.at[i]) for i, (src, dst) in enumerate((
        (gamma_h, gamma_row), (beta_h, beta_row), (wb_h, wb_t), (zin_h, zin), (mask_h, mask),
        (wq_h, w_q), (wk_h, w_k), (wv_h, w_v), (wg_h, w_g), (wo_h, w_o)))]
    for c in loads:
        c.start()

    barrier = pltpu.get_barrier_semaphore()
    for d in range(1, n_col):
        pl.semaphore_signal(barrier, inc=1, device_id={'col': at_col(d)}, device_id_type=MESH)
    for d in range(1, n_row):
        pl.semaphore_signal(barrier, inc=1, device_id={'row': at_row(d)}, device_id_type=MESH)

    for c in loads[:4]:
        c.wait()
    ga = column(gamma_row[...], strip)
    be = column(beta_row[...], strip)
    tile_bias(zin, wb_t[...].astype(F32), ga, be, bt)
    pl.semaphore_wait(barrier, n_col + n_row - 2)

    def keys_of(c):
        return pl.ds(pl.multiple_of(c * cols, cols), cols)

    def first(e, d):
        peer = at_col(d)
        head = lax.rem(peer, 2) * hh + e
        return remote(bt.at[head], ball.at[row, head, keys_of(col), :],
                      b1_send.at[e, d - 1], b1_recv.at[e, d - 1], {'col': peer})

    def second(e, src, c, d):
        head = core * hh + e
        return remote(src, ball.at[row, head, keys_of(c), :],
                      b2_send.at[e, d - 1], b2_recv.at[e, d - 1], {'row': at_row(d)})

    near = (1, n_row - 1)
    for e in range(hh):
        for d in range(1, n_col):
            first(e, d).start()
    for e in range(hh):
        for d in near:
            second(e, bt.at[core * hh + e], col, d).start()

    def rows_out(q, d):
        peer = at_col(d)
        return remote(zt.at[pl.ds(peer * own + q * part, part)], zbuf.at[col, pl.ds(q * part, part)],
                      z_send.at[q, d - 1], z_recv.at[q, d - 1], {'col': peer})

    to_rows(zin, zt)
    for q in range(n_part):
        for d in range(1, n_col):
            rows_out(q, d).start()

    for c in loads[4:]:
        c.wait()
    kb[...] = column(jnp.where(mask[...] > 0, 0.0, -1e9).astype(F32), strip)
    w_t[...] = jnp.concatenate([w[...].astype(F32).T for w in (w_q, w_k, w_v, w_g)], axis=0).astype(BF16)
    wo_t[...] = w_o[...].astype(F32).T.astype(BF16)
    affine[0] = ga
    affine[1] = be
    zbuf[col] = zt[pl.ds(col * own, own)]
    for e in range(hh):
        ball[row, core * hh + e, keys_of(col), :] = bt[core * hh + e]
    for d in range(1, n_col):
        src = lax.rem(col + n_col - d, n_col)
        for e in range(hh):
            first(e, d).wait_recv()
            for f in near:
                second(e, ball.at[row, core * hh + e, keys_of(src), :], src, f).start()

    def third(e, d):
        head = core * hh + e
        from_row = lax.rem(row + n_row - d, n_row)
        return remote(ball.at[from_row, head], ball.at[from_row, head],
                      b3_send.at[e, d], b3_recv.at[e, d], {'col': mate})

    def whole_second(e, d):
        head = core * hh + e
        return remote(ball.at[row, head], ball.at[row, head],
                      b2_send.at[e, d - 1], b2_recv.at[e, d - 1], {'row': at_row(d)})

    def beyond(e):
        d = near[e]
        from_row = lax.rem(row + n_row - d, n_row)
        head = core * hh + e
        return remote(ball.at[from_row, head], ball.at[from_row, head],
                      b2_send.at[e, 1], b2_recv.at[e, 1], {'row': at_row(d)})

    def widen(h, d):
        r = lax.rem(row + n_row - d, n_row)
        pos = (0, 1, n_row - 1, 2).index(d)
        bias[pos // 2, h, :, (pos % 2) * strip:(pos % 2 + 1) * strip] = ball[r, h].astype(F32) + kb[...]

    def arrived(e, d):
        whole_second(e, d).wait_recv()
        third(e, d).start()
        widen(core * hh + e, d)

    def take_rows(q):
        for d in range(1, n_col):
            rows_out(q, d).wait_recv()
        place = [place_of(row, n_row, x) for x in range(n_row)]
        wide = [jnp.concatenate([affine[i]] * (n // strip), axis=1) for i in range(2)]

        def body(r, carry):
            project(r, place, zbuf, w_t[...], wide[0], wide[1], heads, zr, qz, kr, vr, gr)
            return carry

        lax.fori_loop(q * part, (q + 1) * part, body, 0)

    run = functools.partial(step, early=early, n_step=n_step, heads=heads, bias=bias, qz=qz, kr=kr, vr=vr,
                            gr=gr, sref=sref, mref=mref, gat=gat)

    def chips_of(side):
        first_half = [strip_at(row, n_row, p) for p in (0, 1)]
        second_half = [strip_at(row, n_row, p) for p in (2, 3)]
        return [jnp.where(side == 0, a, b) for a, b in zip(first_half, second_half)]

    def make(t):
        pair, side = where_of(t, early)
        for i in range(2):
            finish(2 * pair + i, side, chips_of(side), zr, gat, wo_t[...], heads, obuf)

    def give(t):
        pair, side = where_of(t, early)
        rows = pl.ds(2 * pair, 2)
        for x in chips_of(side):
            for c in range(2):
                peer = 2 * x + c
                d = lax.rem(peer + n_col - col, n_col)

                @pl.when(d > 0)
                def _():
                    remote(obuf.at[peer, rows], res.at[col, rows],
                           o_send.at[d - 1], o_recv.at[d - 1], {'col': peer}).start()

    def other_core(e, d):
        third(e, d).wait_recv()
        widen((1 - core) * hh + e, d)

    up, down = near
    for e in range(hh):
        third(e, 0).start()
        widen(core * hh + e, 0)
    for e in range(hh):
        whole_second(e, near[e]).wait_recv()
        beyond(e).start()
        third(e, near[e]).start()
    whole_second(1, up).wait_recv()
    third(1, up).start()
    take_rows(0)
    for e in range(hh):
        widen(core * hh + e, up)
    for d in (0, up):
        for e in range(hh):
            other_core(e, d)

    run(-1, do_ex=False)
    run(0)

    def body(t, carry):
        @pl.when(t == 1)
        def _():
            take_rows(1)

        @pl.when(t == early - 2)
        def _():
            arrived(0, down)
            widen(core * hh + 1, down)
            for e in range(hh):
                arrived(e, 2)

        @pl.when(t == early - 1)
        def _():
            for d in (down, 2):
                for e in range(hh):
                    other_core(e, d)

        for q in range(2, n_part):
            pl.when(t == q * part - 3)(functools.partial(take_rows, q))

        make(t - 1)
        run(t)
        give(t - 1)
        return carry

    lax.fori_loop(1, n_step, body, 0)
    make(n_step - 1)
    give(n_step - 1)

    mine = pltpu.make_async_copy(obuf.at[col], res.at[col], own_sem)
    mine.start()
    for e in range(hh):
        for d in range(1, n_col):
            first(e, d).wait_send()
        for d in near:
            whole_second(e, d).wait_send()
        beyond(e).wait_send()
        for d in range(n_row):
            third(e, d).wait_send()
    for q in range(n_part):
        for d in range(1, n_col):
            rows_out(q, d).wait_send()
    for d in range(1, n_col):
        peer = at_col(d)
        whole = remote(obuf.at[peer], res.at[col], o_send.at[d - 1], o_recv.at[d - 1], {'col': peer})
        whole.wait_send()
        whole.wait_recv()
    mine.wait()


def solution(mesh):
    n_col = mesh.shape['col']
    n_row = mesh.shape['row']
    tile_spec = P(('dp', 'row'), 'col', None)
    hbm = pl.BlockSpec(memory_space=pltpu.HBM)
    n_part = 4

    def per_device(pair_tile, res_mask, ln_gamma, ln_beta, w_q, w_k, w_v, w_b, w_g, w_o):
        row_len, col_len, chan = pair_tile.shape
        heads = w_b.shape[1]
        hd = chan // heads
        n = res_mask.shape[0]
        own = row_len // n_col
        hc = chan // 2
        lanes = 2 * col_len
        dma = pltpu.SemaphoreType.DMA
        res = pl.pallas_call(
            functools.partial(attn_kernel, n_col, n_row),
            in_specs=[hbm] * 10,
            out_specs=hbm,
            out_shape=jax.ShapeDtypeStruct((n_col, own, hc, lanes), BF16),
            scratch_shapes=[
                pltpu.VMEM((col_len, chan, row_len), BF16),
                pltpu.VMEM((1, n), res_mask.dtype),
                pltpu.VMEM((1, chan), F32),
                pltpu.VMEM((1, chan), F32),
                pltpu.VMEM(w_q.shape, BF16),
                pltpu.VMEM(w_k.shape, BF16),
                pltpu.VMEM(w_v.shape, BF16),
                pltpu.VMEM(w_g.shape, BF16),
                pltpu.VMEM((heads, chan), BF16),
                pltpu.VMEM(w_o.shape, BF16),
                pltpu.VMEM((heads, col_len, row_len), BF16),
                pltpu.VMEM((row_len, hc, lanes), BF16),
                pltpu.VMEM((n_col, own, hc, lanes), BF16),
                pltpu.VMEM((n_row, heads, n, row_len), BF16),
                pltpu.VMEM((2, heads, n, n // 2), F32),
                pltpu.VMEM((n, row_len), F32),
                pltpu.VMEM((2, own, chan, n // 2), F32),
                pltpu.VMEM((2, own * heads, chan, n // 2), BF16),
                pltpu.VMEM((own, n, chan), BF16),
                pltpu.VMEM((own * heads, hd, n), BF16),
                pltpu.VMEM((2, own * heads, hd, n // 2), F32),
                pltpu.VMEM((2 * heads, n, n // 2), F32),
                pltpu.VMEM((2 * heads, 1, n // 2), F32),
                pltpu.VMEM((2, own * heads, hd, n // 2), BF16),
                pltpu.VMEM((n_col, own, hc, lanes), BF16),
                pltpu.VMEM((4 * chan, chan), BF16),
                pltpu.VMEM((chan, chan), BF16),
                pltpu.VMEM((2, chan, row_len), F32),
                dma((10,)),
                dma((heads // 2, n_col - 1)), dma((heads // 2, n_col - 1)),
                dma((n_part, n_col - 1)), dma((n_part, n_col - 1)),
                dma((heads // 2, n_row - 1)), dma((heads // 2, n_row - 1)),
                dma((heads // 2, n_row)), dma((heads // 2, n_row)),
                dma((n_col - 1,)), dma((n_col - 1,)), dma,
            ],
            compiler_params=pltpu.CompilerParams(
                collective_id=0, has_side_effects=True, vmem_limit_bytes=56 << 20),
            name='attention',
        )(jnp.transpose(pair_tile, (1, 2, 0)), res_mask.reshape(1, n), ln_gamma.reshape(1, chan),
          ln_beta.reshape(1, chan), w_q, w_k, w_v, w_g, w_b.T, w_o)

        pairs = 16
        out = pl.pallas_call(
            unpack_kernel,
            grid=(hc // pairs,),
            in_specs=[pl.BlockSpec((row_len, pairs, lanes), lambda i: (0, i, 0))],
            out_specs=pl.BlockSpec((col_len, 2, pairs, row_len), lambda i: (0, 0, i, 0)),
            out_shape=jax.ShapeDtypeStruct((col_len, 2, hc, row_len), BF16),
            name='unpack',
        )(res.reshape(row_len, hc, lanes)).reshape(col_len, chan, row_len)
        return jnp.transpose(out, (2, 0, 1))

    return jax.shard_map(per_device, mesh=mesh,
                         in_specs=(tile_spec, P('dp'), P(), P(), P(), P(), P(), P(), P(), P()),
                         out_specs=tile_spec, check_vma=False)
```

```python
import functools

import jax
import jax.numpy as jnp
from jax import lax
from jax.experimental import pallas as pl
from jax.experimental.pallas import tpu as pltpu
from jax.sharding import PartitionSpec as P

LN_EPS = 1e-5
F32 = jnp.float32
BF16 = jnp.bfloat16
MESH = pl.DeviceIdType.MESH

KEYS = 64
TILE = 256


def column(row, lanes):
    return jnp.broadcast_to(row, (lanes, row.shape[-1])).T


def layer_norm(z, gamma, beta, axis):
    mean = jnp.mean(z, axis=axis, keepdims=True)
    cen = z - mean
    var = jnp.mean(cen * cen, axis=axis, keepdims=True)
    return (cen * lax.rsqrt(var + LN_EPS) * gamma + beta).astype(BF16)


def tile_bias(zin, wb_t, gamma, beta, bt):
    n_key, chan, n_q = zin.shape
    heads = bt.shape[0]
    group = 16
    wide = jnp.concatenate([wb_t, wb_t], axis=1)
    wide = jnp.concatenate([wide] * (group // 2), axis=1)
    rows = jnp.concatenate([jnp.broadcast_to(wide[h:h + 1], (group, group * chan)) for h in range(heads)], axis=0)
    own = lax.broadcasted_iota(jnp.int32, rows.shape, 0) % group
    src = lax.broadcasted_iota(jnp.int32, rows.shape, 1) // chan
    big = jnp.where(own == src, rows, 0.0).astype(BF16)

    def body(g, carry):
        start = pl.multiple_of(g * group, group)
        normed = layer_norm(zin[pl.ds(start, group)].astype(F32), gamma[None], beta[None], 1)
        out = jnp.dot(big, normed.reshape(group * chan, n_q), preferred_element_type=F32)
        for h in range(heads):
            bt[h, pl.ds(start, group), :] = out[h * group:(h + 1) * group].astype(BF16)
        return carry

    lax.fori_loop(0, n_key // group, body, 0)


def to_rows(zin, zt):
    n_key, chan, _ = zin.shape
    hc = chan // 2
    for s in range(0, hc, 16):
        a = jnp.swapaxes(zin[:, s:s + 16, :].astype(F32), 0, 1)
        b = jnp.swapaxes(zin[:, hc + s:hc + s + 16, :].astype(F32), 0, 1)
        c = jnp.concatenate([a, b], axis=1)
        c = jnp.stack([c[i].T for i in range(16)], axis=0)
        zt[:, s:s + 16, :] = jnp.swapaxes(c, 0, 1).astype(BF16)


def unpack_kernel(r, out):
    n_key = out.shape[0]
    pairs = r.shape[1]
    c = jnp.swapaxes(r[...].astype(F32), 0, 1)
    c = [c[i].T for i in range(pairs)]
    for half in range(2):
        x = jnp.stack([y[half * n_key:(half + 1) * n_key] for y in c], axis=0)
        out[:, half] = jnp.swapaxes(x, 0, 1).astype(BF16)


def strip_at(row, n_row, pos):
    return lax.rem(row + n_row - jnp.where(pos < 2, pos, n_row + 1 - pos), n_row)


def place_of(row, n_row, strip):
    back = lax.rem(row + n_row - strip, n_row)
    return jnp.where(back < 2, back, n_row + 1 - back)


def project(r, place, zbuf, w_t, gamma, beta, heads, zr, qz, kr, vr, gr):
    n_src, _, hc, lanes = zbuf.shape
    chan = 2 * hc
    half = lanes // 2
    n = n_src * half
    hd = chan // heads
    low = lax.broadcasted_iota(jnp.int32, (hc, lanes), 1) < half
    cols = []
    for x in range(n_src // 2):
        a = zbuf[2 * x, r].astype(F32)
        b = zbuf[2 * x + 1, r].astype(F32)
        top = jnp.where(low, a, pltpu.roll(b, half, 1))
        bot = jnp.where(low, pltpu.roll(a, half, 1), b)
        cols.append(jnp.concatenate([top, bot], axis=0))
    z = jnp.concatenate(cols, axis=1)
    proj = jnp.dot(w_t, layer_norm(z, gamma, beta, 0), preferred_element_type=F32)
    q_t = (proj[:chan] * hd ** -0.5).astype(BF16)
    gates = jax.nn.sigmoid(proj[3 * chan:])
    hh = heads // 2
    for x, pos in enumerate(place):
        cs = slice(x * lanes, (x + 1) * lanes)
        zr[pos, r] = z[:, cs]
        for p in range(hh):
            both = []
            for h in (2 * p, 2 * p + 1):
                parts = []
                if h > 0:
                    parts.append(jnp.zeros((h * hd, lanes), BF16))
                parts.append(q_t[h * hd:(h + 1) * hd, cs])
                if h < heads - 1:
                    parts.append(jnp.zeros(((heads - 1 - h) * hd, lanes), BF16))
                both.append(jnp.concatenate(parts, axis=0))
            qz[pos, r * hh + p] = jnp.concatenate(both, axis=1)
            gr[pos, r * hh + p] = jnp.concatenate(
                [gates[h * hd:(h + 1) * hd, cs] for h in (2 * p, 2 * p + 1)], axis=1)
    for p in range(hh):
        vr[r * hh + p] = proj[2 * chan + 2 * p * hd:2 * chan + 2 * (p + 1) * hd].astype(BF16)
    kr[r] = proj[chan:2 * chan].T.astype(BF16)


class Logits:
    def __init__(self, slot, pos, row, pair, hh, bias, qz, kr, sref, mref):
        self.slot, self.pos, self.pair, self.bias, self.sref, self.mref = slot, pos, pair, bias, sref, mref
        self.value = jnp.dot(kr[row], qz[pos, row * hh + pair], preferred_element_type=F32)
        self.top = None
        self.done = 0

    def advance(self):
        _, n, width = self.sref.shape
        if self.done == n:
            return
        sl = slice(self.done, self.done + KEYS)
        self.done += KEYS
        part = self.value[sl] + self.bias[self.pos, self.pair, sl, :]
        self.sref[self.slot, sl, :] = part
        top = jnp.max(part.reshape(KEYS // 8, 8, width), axis=0)
        self.top = top if self.top is None else jnp.maximum(self.top, top)

    def end(self):
        while self.done < self.sref.shape[1]:
            self.advance()
        self.mref[self.slot] = jnp.max(self.top, axis=0, keepdims=True)


def where_of(t, n_group):
    u = t - n_group
    v = u - 6
    group = jnp.where(u < 0, t, jnp.where(u < 4, u // 2, jnp.where(u < 6, u - 4, 2 + v // 3)))
    pos = jnp.where(u < 0, 0, jnp.where(u < 4, 1 + u % 2, jnp.where(u < 6, 3, 1 + v % 3)))
    return group, pos


def step(t, n_group, n_step, hh, bias, qz, kr, vr, gr, sref, mref, gat, do_ex=True):
    slots, n, width = sref.shape
    rows = slots // hh
    nxt = t + 1 if isinstance(t, int) else jnp.minimum(t + 1, n_step - 1)
    n_row, n_pos = where_of(nxt, n_group)
    row, pos = where_of(t, n_group)
    pending = None
    for i in range(slots):
        logits = Logits(i, n_pos, rows * n_row + i // hh, i % hh, hh, bias, qz, kr, sref, mref)
        if do_ex:
            idx = (rows * row + i // hh) * hh + i % hh
            v = vr[idx]
            hd = v.shape[0] // 2
            peak = jnp.broadcast_to(mref[i], (8, width))[None]
            total = jnp.zeros((8, width), F32)
            acc = None
            for k0 in range(0, n, TILE):
                parts = []
                for k1 in range(k0, k0 + TILE, KEYS):
                    p = jnp.exp(sref[i, k1:k1 + KEYS].reshape(KEYS // 8, 8, width) - peak)
                    total = total + jnp.sum(p, axis=0)
                    parts.append(p.reshape(KEYS, width).astype(BF16))
                    if pending is not None:
                        pending.advance()
                d = jnp.dot(v[:, k0:k0 + TILE], jnp.concatenate(parts, axis=0), preferred_element_type=F32)
                acc = d if acc is None else acc + d
            acc = jnp.concatenate([acc[:hd, :width // 2], acc[hd:, width // 2:]], axis=1)
            gat[pos, idx] = (gr[pos, idx] * (acc / jnp.sum(total, axis=0, keepdims=True))).astype(BF16)
        if pending is not None:
            pending.end()
        pending = logits
    pending.end()


def finish(row0, rows, pos, chip, zr, gat, wo_t, heads, obuf):
    _, _, hc, lanes = obuf.shape
    hh = heads // 2
    half = lanes // 2
    low = lax.broadcasted_iota(jnp.int32, (hc, lanes), 1) < half
    gated = jnp.concatenate([
        jnp.concatenate([gat[pos, (row0 + i) * hh + h // 2][:, (h % 2) * lanes:(h % 2 + 1) * lanes]
                         for h in range(heads)], axis=0) for i in range(rows)], axis=1)
    update = jnp.dot(wo_t, gated, preferred_element_type=F32)
    for i in range(rows):
        o = zr[pos, row0 + i] + update[:, i * lanes:(i + 1) * lanes]
        top = o[:hc]
        bot = o[hc:]
        obuf[2 * chip, row0 + i] = jnp.where(low, top, pltpu.roll(bot, half, 1)).astype(BF16)
        obuf[2 * chip + 1, row0 + i] = jnp.where(low, pltpu.roll(top, half, 1), bot).astype(BF16)


def attn_kernel(n_col, n_row, zin_h, mask_h, gamma_h, beta_h, wq_h, wk_h, wv_h, wg_h, wb_h, wo_h, res,
                zin, mask, gamma_row, beta_row, w_q, w_k, w_v, w_g, wb_t, w_o,
                bt, zt, zbuf, ball, bias, kb, zr, qz, kr, vr, gr, sref, mref, gat, obuf, w_t, wo_t, affine,
                in_sem, b1_send, b1_recv, z_send, z_recv, b2_send, b2_recv, b3_send, b3_recv,
                o_send, o_recv, own_sem):
    col = lax.axis_index('col')
    row = lax.axis_index('row')
    core = lax.rem(col, 2)
    mate = col + 1 - 2 * core
    heads, cols, strip = bt.shape
    hh = heads // 2
    own = zbuf.shape[1]
    n = sref.shape[1]
    n_part = z_send.shape[0]
    part = own // n_part
    n_group = n_part
    n_step = n_group * n_row

    def at_col(d):
        return lax.rem(col + d, n_col)

    def at_row(d):
        return lax.rem(row + d, n_row)

    def remote(src, dst, send, recv, where):
        return pltpu.make_async_remote_copy(src_ref=src, dst_ref=dst, send_sem=send, recv_sem=recv,
                                            device_id=where, device_id_type=MESH)

    loads = [pltpu.make_async_copy(src, dst, in_sem.at[i]) for i, (src, dst) in enumerate((
        (gamma_h, gamma_row), (beta_h, beta_row), (wb_h, wb_t), (zin_h, zin), (mask_h, mask),
        (wq_h, w_q), (wk_h, w_k), (wv_h, w_v), (wg_h, w_g), (wo_h, w_o)))]
    for c in loads:
        c.start()

    barrier = pltpu.get_barrier_semaphore()
    for d in range(1, n_col):
        pl.semaphore_signal(barrier, inc=1, device_id={'col': at_col(d)}, device_id_type=MESH)
    for d in range(1, n_row):
        pl.semaphore_signal(barrier, inc=1, device_id={'row': at_row(d)}, device_id_type=MESH)

    for c in loads[:4]:
        c.wait()
    ga = column(gamma_row[...], strip)
    be = column(beta_row[...], strip)
    tile_bias(zin, wb_t[...].astype(F32), ga, be, bt)
    pl.semaphore_wait(barrier, n_col + n_row - 2)

    def keys_of(c):
        return pl.ds(pl.multiple_of(c * cols, cols), cols)

    def first(e, d):
        peer = at_col(d)
        head = lax.rem(peer, 2) * hh + e
        return remote(bt.at[head], ball.at[row, head, keys_of(col), :],
                      b1_send.at[e, d - 1], b1_recv.at[e, d - 1], {'col': peer})

    def second(e, src, c, d):
        head = core * hh + e
        return remote(src, ball.at[row, head, keys_of(c), :],
                      b2_send.at[e, d - 1], b2_recv.at[e, d - 1], {'row': at_row(d)})

    near = (1, n_row - 1)
    for e in range(hh):
        for d in range(1, n_col):
            first(e, d).start()
    for e in range(hh):
        for d in near:
            second(e, bt.at[core * hh + e], col, d).start()

    def rows_out(q, d):
        peer = at_col(d)
        return remote(zt.at[pl.ds(peer * own + q * part, part)], zbuf.at[col, pl.ds(q * part, part)],
                      z_send.at[q, d - 1], z_recv.at[q, d - 1], {'col': peer})

    to_rows(zin, zt)
    def send_part(q):
        for d in range(1, n_col):
            rows_out(q, d).start()

    send_part(0)
    send_part(1)

    for c in loads[4:]:
        c.wait()
    kb[...] = column(jnp.where(mask[...] > 0, 0.0, -1e9).astype(F32), strip)
    w_t[...] = jnp.concatenate([w[...].astype(F32).T for w in (w_q, w_k, w_v, w_g)], axis=0).astype(BF16)
    wo_t[...] = w_o[...].astype(F32).T.astype(BF16)
    affine[0] = ga
    affine[1] = be
    zbuf[col] = zt[pl.ds(col * own, own)]
    for e in range(hh):
        ball[row, core * hh + e, keys_of(col), :] = bt[core * hh + e]
    for d in range(1, n_col):
        src = lax.rem(col + n_col - d, n_col)
        for e in range(hh):
            first(e, d).wait_recv()
            for f in near:
                second(e, ball.at[row, core * hh + e, keys_of(src), :], src, f).start()

    send_part(2)

    def third(e, d):
        head = core * hh + e
        from_row = lax.rem(row + n_row - d, n_row)
        return remote(ball.at[from_row, head], ball.at[from_row, head],
                      b3_send.at[e, d], b3_recv.at[e, d], {'col': mate})

    def whole_second(e, d):
        head = core * hh + e
        return remote(ball.at[row, head], ball.at[row, head],
                      b2_send.at[e, d - 1], b2_recv.at[e, d - 1], {'row': at_row(d)})

    def beyond(e):
        d = near[e]
        from_row = lax.rem(row + n_row - d, n_row)
        head = core * hh + e
        return remote(ball.at[from_row, head], ball.at[from_row, head],
                      b2_send.at[e, 1], b2_recv.at[e, 1], {'row': at_row(d)})

    def widen(side, e, d):
        r = lax.rem(row + n_row - d, n_row)
        pos = (0, 1, n_row - 1, 2).index(d)
        bias[pos, side, :, e * strip:(e + 1) * strip] = ball[r, side * hh + e].astype(F32) + kb[...]

    def arrived(e, d):
        whole_second(e, d).wait_recv()
        third(e, d).start()

    def complete(d):
        for e in range(hh):
            widen(core, e, d)
        for e in range(hh):
            third(e, d).wait_recv()
            widen(1 - core, e, d)

    def take_rows(q):
        for d in range(1, n_col):
            rows_out(q, d).wait_recv()
        place = [place_of(row, n_row, x) for x in range(n_row)]
        wide = [jnp.concatenate([affine[i]] * (n // strip), axis=1) for i in range(2)]

        def body(r, carry):
            project(r, place, zbuf, w_t[...], wide[0], wide[1], heads, zr, qz, kr, vr, gr)
            return carry

        lax.fori_loop(q * part, (q + 1) * part, body, 0)

    run = functools.partial(step, n_group=n_group, n_step=n_step, hh=hh, bias=bias, qz=qz, kr=kr, vr=vr,
                            gr=gr, sref=sref, mref=mref, gat=gat)

    def make(t):
        group, pos = where_of(t, n_group)
        finish(group * part, part, pos, strip_at(row, n_row, pos), zr, gat, wo_t[...], heads, obuf)

    def give(t):
        group, pos = where_of(t, n_group)
        rows = pl.ds(group * part, part)
        for c in range(2):
            peer = 2 * strip_at(row, n_row, pos) + c
            d = lax.rem(peer + n_col - col, n_col)

            @pl.when(d > 0)
            def _():
                remote(obuf.at[peer, rows], res.at[col, rows],
                       o_send.at[d - 1], o_recv.at[d - 1], {'col': peer}).start()

    up, down = near
    for e in range(hh):
        third(e, 0).start()
    take_rows(0)
    complete(0)
    send_part(3)
    run(-1, do_ex=False)
    take_rows(1)
    run(0)

    def body(t, carry):
        @pl.when(t == 1)
        def _():
            take_rows(2)

        @pl.when(t == 2)
        def _():
            for e in range(hh):
                whole_second(e, near[e]).wait_recv()
                beyond(e).start()
            for e in range(hh):
                third(e, near[e]).start()
                arrived(e, near[1 - e])
            take_rows(3)

        @pl.when(t == 3)
        def _():
            complete(up)

        @pl.when(t == 4)
        def _():
            complete(down)

        @pl.when(t == 6)
        def _():
            for e in range(hh):
                arrived(e, 2)

        @pl.when(t == 7)
        def _():
            complete(2)

        make(t - 1)
        run(t)
        give(t - 1)
        return carry

    lax.fori_loop(1, n_step, body, 0)
    make(n_step - 1)
    give(n_step - 1)

    mine = pltpu.make_async_copy(obuf.at[col], res.at[col], own_sem)
    mine.start()
    for e in range(hh):
        for d in range(1, n_col):
            first(e, d).wait_send()
        for d in near:
            whole_second(e, d).wait_send()
        beyond(e).wait_send()
        for d in range(n_row):
            third(e, d).wait_send()
    for q in range(n_part):
        for d in range(1, n_col):
            rows_out(q, d).wait_send()
    for d in range(1, n_col):
        peer = at_col(d)
        whole = remote(obuf.at[peer], res.at[col], o_send.at[d - 1], o_recv.at[d - 1], {'col': peer})
        whole.wait_send()
        whole.wait_recv()
    mine.wait()


def solution(mesh):
    n_col = mesh.shape['col']
    n_row = mesh.shape['row']
    tile_spec = P(('dp', 'row'), 'col', None)
    hbm = pl.BlockSpec(memory_space=pltpu.HBM)
    n_part = 4

    def per_device(pair_tile, res_mask, ln_gamma, ln_beta, w_q, w_k, w_v, w_b, w_g, w_o):
        row_len, col_len, chan = pair_tile.shape
        heads = w_b.shape[1]
        hd = chan // heads
        n = res_mask.shape[0]
        own = row_len // n_col
        hc = chan // 2
        lanes = 2 * col_len
        dma = pltpu.SemaphoreType.DMA
        res = pl.pallas_call(
            functools.partial(attn_kernel, n_col, n_row),
            in_specs=[hbm] * 10,
            out_specs=hbm,
            out_shape=jax.ShapeDtypeStruct((n_col, own, hc, lanes), BF16),
            scratch_shapes=[
                pltpu.VMEM((col_len, chan, row_len), BF16),
                pltpu.VMEM((1, n), res_mask.dtype),
                pltpu.VMEM((1, chan), F32),
                pltpu.VMEM((1, chan), F32),
                pltpu.VMEM(w_q.shape, BF16),
                pltpu.VMEM(w_k.shape, BF16),
                pltpu.VMEM(w_v.shape, BF16),
                pltpu.VMEM(w_g.shape, BF16),
                pltpu.VMEM((heads, chan), BF16),
                pltpu.VMEM(w_o.shape, BF16),
                pltpu.VMEM((heads, col_len, row_len), BF16),
                pltpu.VMEM((row_len, hc, lanes), BF16),
                pltpu.VMEM((n_col, own, hc, lanes), BF16),
                pltpu.VMEM((n_row, heads, n, row_len), BF16),
                pltpu.VMEM((n_row, heads // 2, n, 2 * row_len), F32),
                pltpu.VMEM((n, row_len), F32),
                pltpu.VMEM((n_row, own, chan, row_len), F32),
                pltpu.VMEM((n_row, own * heads // 2, chan, 2 * row_len), BF16),
                pltpu.VMEM((own, n, chan), BF16),
                pltpu.VMEM((own * heads // 2, 2 * hd, n), BF16),
                pltpu.VMEM((n_row, own * heads // 2, hd, 2 * row_len), F32),
                pltpu.VMEM((own // n_part * heads // 2, n, 2 * row_len), F32),
                pltpu.VMEM((own // n_part * heads // 2, 1, 2 * row_len), F32),
                pltpu.VMEM((n_row, own * heads // 2, hd, 2 * row_len), BF16),
                pltpu.VMEM((n_col, own, hc, lanes), BF16),
                pltpu.VMEM((4 * chan, chan), BF16),
                pltpu.VMEM((chan, chan), BF16),
                pltpu.VMEM((2, chan, row_len), F32),
                dma((10,)),
                dma((heads // 2, n_col - 1)), dma((heads // 2, n_col - 1)),
                dma((n_part, n_col - 1)), dma((n_part, n_col - 1)),
                dma((heads // 2, n_row - 1)), dma((heads // 2, n_row - 1)),
                dma((heads // 2, n_row)), dma((heads // 2, n_row)),
                dma((n_col - 1,)), dma((n_col - 1,)), dma,
            ],
            compiler_params=pltpu.CompilerParams(
                collective_id=0, has_side_effects=True, vmem_limit_bytes=56 << 20),
            name='attention',
        )(jnp.transpose(pair_tile, (1, 2, 0)), res_mask.reshape(1, n), ln_gamma.reshape(1, chan),
          ln_beta.reshape(1, chan), w_q, w_k, w_v, w_g, w_b.T, w_o)

        pairs = 16
        out = pl.pallas_call(
            unpack_kernel,
            grid=(hc // pairs,),
            in_specs=[pl.BlockSpec((row_len, pairs, lanes), lambda i: (0, i, 0))],
            out_specs=pl.BlockSpec((col_len, 2, pairs, row_len), lambda i: (0, 0, i, 0)),
            out_shape=jax.ShapeDtypeStruct((col_len, 2, hc, row_len), BF16),
            name='unpack',
        )(res.reshape(row_len, hc, lanes)).reshape(col_len, chan, row_len)
        return jnp.transpose(out, (2, 0, 1))

    return jax.shard_map(per_device, mesh=mesh,
                         in_specs=(tile_spec, P('dp'), P(), P(), P(), P(), P(), P(), P(), P()),
                         out_specs=tile_spec, check_vma=False)
```

```python
import functools

import jax
import jax.numpy as jnp
from jax import lax
from jax.experimental import pallas as pl
from jax.experimental.pallas import tpu as pltpu
from jax.sharding import PartitionSpec as P

LN_EPS = 1e-5
F32 = jnp.float32
BF16 = jnp.bfloat16
MESH = pl.DeviceIdType.MESH

KEYS = 64
TILE = 256


def column(row, lanes):
    return jnp.broadcast_to(row, (lanes, row.shape[-1])).T


def layer_norm(z, gamma, beta, axis):
    mean = jnp.mean(z, axis=axis, keepdims=True)
    cen = z - mean
    var = jnp.mean(cen * cen, axis=axis, keepdims=True)
    return (cen * lax.rsqrt(var + LN_EPS) * gamma + beta).astype(BF16)


def tile_bias(zin, wb_t, gamma, beta, bt):
    n_key, chan, n_q = zin.shape
    heads = bt.shape[0]
    group = 16
    wide = jnp.concatenate([wb_t, wb_t], axis=1)
    wide = jnp.concatenate([wide] * (group // 2), axis=1)
    rows = jnp.concatenate([jnp.broadcast_to(wide[h:h + 1], (group, group * chan)) for h in range(heads)], axis=0)
    own = lax.broadcasted_iota(jnp.int32, rows.shape, 0) % group
    src = lax.broadcasted_iota(jnp.int32, rows.shape, 1) // chan
    big = jnp.where(own == src, rows, 0.0).astype(BF16)

    def body(g, carry):
        start = pl.multiple_of(g * group, group)
        normed = layer_norm(zin[pl.ds(start, group)].astype(F32), gamma[None], beta[None], 1)
        out = jnp.dot(big, normed.reshape(group * chan, n_q), preferred_element_type=F32)
        for h in range(heads):
            bt[h, pl.ds(start, group), :] = out[h * group:(h + 1) * group].astype(BF16)
        return carry

    lax.fori_loop(0, n_key // group, body, 0)


def to_rows(zin, zt):
    n_key, chan, _ = zin.shape
    hc = chan // 2
    for s in range(0, hc, 16):
        a = jnp.swapaxes(zin[:, s:s + 16, :].astype(F32), 0, 1)
        b = jnp.swapaxes(zin[:, hc + s:hc + s + 16, :].astype(F32), 0, 1)
        c = jnp.concatenate([a, b], axis=1)
        c = jnp.stack([c[i].T for i in range(16)], axis=0)
        zt[:, s:s + 16, :] = jnp.swapaxes(c, 0, 1).astype(BF16)


def unpack_kernel(r, out):
    n_key = out.shape[0]
    pairs = r.shape[1]
    c = jnp.swapaxes(r[...].astype(F32), 0, 1)
    c = [c[i].T for i in range(pairs)]
    for half in range(2):
        x = jnp.stack([y[half * n_key:(half + 1) * n_key] for y in c], axis=0)
        out[:, half] = jnp.swapaxes(x, 0, 1).astype(BF16)


def strip_at(row, n_row, pos):
    return lax.rem(row + n_row - jnp.where(pos < 2, pos, n_row + 1 - pos), n_row)


def place_of(row, n_row, strip):
    back = lax.rem(row + n_row - strip, n_row)
    return jnp.where(back < 2, back, n_row + 1 - back)


def project(r, place, zbuf, w_t, gamma, beta, heads, zr, qz, kr, vr, gr):
    n_src, _, hc, lanes = zbuf.shape
    chan = 2 * hc
    half = lanes // 2
    n = n_src * half
    hd = chan // heads
    low = lax.broadcasted_iota(jnp.int32, (hc, lanes), 1) < half
    cols = []
    for x in range(n_src // 2):
        a = zbuf[2 * x, r].astype(F32)
        b = zbuf[2 * x + 1, r].astype(F32)
        top = jnp.where(low, a, pltpu.roll(b, half, 1))
        bot = jnp.where(low, pltpu.roll(a, half, 1), b)
        cols.append(jnp.concatenate([top, bot], axis=0))
    z = jnp.concatenate(cols, axis=1)
    proj = jnp.dot(w_t, layer_norm(z, gamma, beta, 0), preferred_element_type=F32)
    q_t = (proj[:chan] * hd ** -0.5).astype(BF16)
    gates = jax.nn.sigmoid(proj[3 * chan:])
    hh = heads // 2
    for x, pos in enumerate(place):
        cs = slice(x * lanes, (x + 1) * lanes)
        zr[pos, r] = z[:, cs]
        for p in range(hh):
            both = []
            for h in (2 * p, 2 * p + 1):
                parts = []
                if h > 0:
                    parts.append(jnp.zeros((h * hd, lanes), BF16))
                parts.append(q_t[h * hd:(h + 1) * hd, cs])
                if h < heads - 1:
                    parts.append(jnp.zeros(((heads - 1 - h) * hd, lanes), BF16))
                both.append(jnp.concatenate(parts, axis=0))
            qz[pos, r * hh + p] = jnp.concatenate(both, axis=1)
            gr[pos, r * hh + p] = jnp.concatenate(
                [gates[h * hd:(h + 1) * hd, cs] for h in (2 * p, 2 * p + 1)], axis=1)
    for p in range(hh):
        vr[r * hh + p] = proj[2 * chan + 2 * p * hd:2 * chan + 2 * (p + 1) * hd].astype(BF16)
    kr[r] = proj[chan:2 * chan].T.astype(BF16)


class Logits:
    def __init__(self, slot, pos, row, pair, hh, bias, qz, kr, sref, mref):
        self.slot, self.pos, self.pair, self.bias, self.sref, self.mref = slot, pos, pair, bias, sref, mref
        self.value = jnp.dot(kr[row], qz[pos, row * hh + pair], preferred_element_type=F32)
        self.top = None
        self.done = 0

    def advance(self):
        _, n, width = self.sref.shape
        if self.done == n:
            return
        sl = slice(self.done, self.done + KEYS)
        self.done += KEYS
        part = self.value[sl] + self.bias[self.pos, self.pair, sl, :]
        self.sref[self.slot, sl, :] = part
        top = jnp.max(part.reshape(KEYS // 8, 8, width), axis=0)
        self.top = top if self.top is None else jnp.maximum(self.top, top)

    def end(self):
        while self.done < self.sref.shape[1]:
            self.advance()
        self.mref[self.slot] = jnp.max(self.top, axis=0, keepdims=True)


ORDER = ((0, 0), (1, 0), (2, 0), (0, 1), (0, 2), (1, 1), (1, 2), (3, 0),
         (0, 3), (1, 3), (2, 1), (2, 2), (2, 3), (3, 1), (3, 2), (3, 3))


def where_of(t):
    group, pos = ORDER[0]
    for i in range(1, len(ORDER)):
        group = jnp.where(t == i, ORDER[i][0], group)
        pos = jnp.where(t == i, ORDER[i][1], pos)
    return group, pos


def step(t, n_step, hh, bias, qz, kr, vr, gr, sref, mref, gat, do_ex=True):
    slots, n, width = sref.shape
    rows = slots // hh
    nxt = t + 1 if isinstance(t, int) else jnp.minimum(t + 1, n_step - 1)
    n_row, n_pos = where_of(nxt)
    row, pos = where_of(t)
    pending = None
    for i in range(slots):
        logits = Logits(i, n_pos, rows * n_row + i // hh, i % hh, hh, bias, qz, kr, sref, mref)
        if do_ex:
            idx = (rows * row + i // hh) * hh + i % hh
            v = vr[idx]
            hd = v.shape[0] // 2
            peak = jnp.broadcast_to(mref[i], (8, width))[None]
            total = jnp.zeros((8, width), F32)
            acc = None
            for k0 in range(0, n, TILE):
                parts = []
                for k1 in range(k0, k0 + TILE, KEYS):
                    p = jnp.exp(sref[i, k1:k1 + KEYS].reshape(KEYS // 8, 8, width) - peak)
                    total = total + jnp.sum(p, axis=0)
                    parts.append(p.reshape(KEYS, width).astype(BF16))
                    if pending is not None:
                        pending.advance()
                d = jnp.dot(v[:, k0:k0 + TILE], jnp.concatenate(parts, axis=0), preferred_element_type=F32)
                acc = d if acc is None else acc + d
            acc = jnp.concatenate([acc[:hd, :width // 2], acc[hd:, width // 2:]], axis=1)
            gat[pos, idx] = (gr[pos, idx] * (acc / jnp.sum(total, axis=0, keepdims=True))).astype(BF16)
        if pending is not None:
            pending.end()
        pending = logits
    pending.end()


def finish(row0, rows, pos, chip, zr, gat, wo_t, heads, obuf):
    _, _, hc, lanes = obuf.shape
    hh = heads // 2
    half = lanes // 2
    low = lax.broadcasted_iota(jnp.int32, (hc, lanes), 1) < half
    gated = jnp.concatenate([
        jnp.concatenate([gat[pos, (row0 + i) * hh + h // 2][:, (h % 2) * lanes:(h % 2 + 1) * lanes]
                         for h in range(heads)], axis=0) for i in range(rows)], axis=1)
    update = jnp.dot(wo_t, gated, preferred_element_type=F32)
    for i in range(rows):
        o = zr[pos, row0 + i] + update[:, i * lanes:(i + 1) * lanes]
        top = o[:hc]
        bot = o[hc:]
        obuf[2 * chip, row0 + i] = jnp.where(low, top, pltpu.roll(bot, half, 1)).astype(BF16)
        obuf[2 * chip + 1, row0 + i] = jnp.where(low, pltpu.roll(top, half, 1), bot).astype(BF16)


def attn_kernel(n_col, n_row, zin_h, mask_h, gamma_h, beta_h, wq_h, wk_h, wv_h, wg_h, wb_h, wo_h, res,
                zin, mask, gamma_row, beta_row, w_q, w_k, w_v, w_g, wb_t, w_o,
                bt, zt, zbuf, ball, bias, kb, zr, qz, kr, vr, gr, sref, mref, gat, obuf, w_t, wo_t, affine,
                in_sem, b1_send, b1_recv, z_send, z_recv, b2_send, b2_recv, b3_send, b3_recv,
                o_send, o_recv, own_sem):
    col = lax.axis_index('col')
    row = lax.axis_index('row')
    core = lax.rem(col, 2)
    mate = col + 1 - 2 * core
    heads, cols, strip = bt.shape
    hh = heads // 2
    own = zbuf.shape[1]
    n = sref.shape[1]
    n_part = z_send.shape[0]
    part = own // n_part
    n_step = len(ORDER)
    assert n_step == n_part * n_row

    def at_col(d):
        return lax.rem(col + d, n_col)

    def at_row(d):
        return lax.rem(row + d, n_row)

    def remote(src, dst, send, recv, where):
        return pltpu.make_async_remote_copy(src_ref=src, dst_ref=dst, send_sem=send, recv_sem=recv,
                                            device_id=where, device_id_type=MESH)

    loads = [pltpu.make_async_copy(src, dst, in_sem.at[i]) for i, (src, dst) in enumerate((
        (gamma_h, gamma_row), (beta_h, beta_row), (wb_h, wb_t), (zin_h, zin), (mask_h, mask),
        (wq_h, w_q), (wk_h, w_k), (wv_h, w_v), (wg_h, w_g), (wo_h, w_o)))]
    for c in loads:
        c.start()

    barrier = pltpu.get_barrier_semaphore()
    for d in range(1, n_col):
        pl.semaphore_signal(barrier, inc=1, device_id={'col': at_col(d)}, device_id_type=MESH)
    for d in range(1, n_row):
        pl.semaphore_signal(barrier, inc=1, device_id={'row': at_row(d)}, device_id_type=MESH)

    for c in loads[:4]:
        c.wait()
    ga = column(gamma_row[...], strip)
    be = column(beta_row[...], strip)
    tile_bias(zin, wb_t[...].astype(F32), ga, be, bt)
    pl.semaphore_wait(barrier, n_col + n_row - 2)

    def keys_of(c):
        return pl.ds(pl.multiple_of(c * cols, cols), cols)

    def first(e, d):
        peer = at_col(d)
        head = lax.rem(peer, 2) * hh + e
        return remote(bt.at[head], ball.at[row, head, keys_of(col), :],
                      b1_send.at[e, d - 1], b1_recv.at[e, d - 1], {'col': peer})

    def second(e, src, c, d):
        head = core * hh + e
        return remote(src, ball.at[row, head, keys_of(c), :],
                      b2_send.at[e, d - 1], b2_recv.at[e, d - 1], {'row': at_row(d)})

    near = (1, n_row - 1)
    for e in range(hh):
        for d in range(1, n_col):
            first(e, d).start()
    for e in range(hh):
        for d in near:
            second(e, bt.at[core * hh + e], col, d).start()

    def rows_out(q, d):
        peer = at_col(d)
        return remote(zt.at[pl.ds(peer * own + q * part, part)], zbuf.at[col, pl.ds(q * part, part)],
                      z_send.at[q, d - 1], z_recv.at[q, d - 1], {'col': peer})

    to_rows(zin, zt)
    def send_part(q):
        for d in range(1, n_col):
            rows_out(q, d).start()

    send_part(0)

    for c in loads[4:]:
        c.wait()
    kb[...] = column(jnp.where(mask[...] > 0, 0.0, -1e9).astype(F32), strip)
    w_t[...] = jnp.concatenate([w[...].astype(F32).T for w in (w_q, w_k, w_v, w_g)], axis=0).astype(BF16)
    wo_t[...] = w_o[...].astype(F32).T.astype(BF16)
    affine[0] = ga
    affine[1] = be
    zbuf[col] = zt[pl.ds(col * own, own)]
    for e in range(hh):
        ball[row, core * hh + e, keys_of(col), :] = bt[core * hh + e]
    for d in range(1, n_col):
        src = lax.rem(col + n_col - d, n_col)
        for e in range(hh):
            first(e, d).wait_recv()
            for f in near:
                second(e, ball.at[row, core * hh + e, keys_of(src), :], src, f).start()

    send_part(1)

    def third(e, d):
        head = core * hh + e
        from_row = lax.rem(row + n_row - d, n_row)
        return remote(ball.at[from_row, head], ball.at[from_row, head],
                      b3_send.at[e, d], b3_recv.at[e, d], {'col': mate})

    def whole_second(e, d):
        head = core * hh + e
        return remote(ball.at[row, head], ball.at[row, head],
                      b2_send.at[e, d - 1], b2_recv.at[e, d - 1], {'row': at_row(d)})

    def beyond(e):
        d = near[e]
        from_row = lax.rem(row + n_row - d, n_row)
        head = core * hh + e
        return remote(ball.at[from_row, head], ball.at[from_row, head],
                      b2_send.at[e, 1], b2_recv.at[e, 1], {'row': at_row(d)})

    def widen(side, e, d):
        r = lax.rem(row + n_row - d, n_row)
        pos = (0, 1, n_row - 1, 2).index(d)
        bias[pos, side, :, e * strip:(e + 1) * strip] = ball[r, side * hh + e].astype(F32) + kb[...]

    def arrived(e, d):
        whole_second(e, d).wait_recv()
        third(e, d).start()

    def complete(d):
        for e in range(hh):
            widen(core, e, d)
        for e in range(hh):
            third(e, d).wait_recv()
            widen(1 - core, e, d)

    def take_rows(q):
        for d in range(1, n_col):
            rows_out(q, d).wait_recv()
        place = [place_of(row, n_row, x) for x in range(n_row)]
        wide = [jnp.concatenate([affine[i]] * (n // strip), axis=1) for i in range(2)]

        def body(r, carry):
            project(r, place, zbuf, w_t[...], wide[0], wide[1], heads, zr, qz, kr, vr, gr)
            return carry

        lax.fori_loop(q * part, (q + 1) * part, body, 0)

    run = functools.partial(step, n_step=n_step, hh=hh, bias=bias, qz=qz, kr=kr, vr=vr,
                            gr=gr, sref=sref, mref=mref, gat=gat)

    def make(t):
        group, pos = where_of(t)
        finish(group * part, part, pos, strip_at(row, n_row, pos), zr, gat, wo_t[...], heads, obuf)

    def give(t):
        group, pos = where_of(t)
        rows = pl.ds(group * part, part)
        for c in range(2):
            peer = 2 * strip_at(row, n_row, pos) + c
            d = lax.rem(peer + n_col - col, n_col)

            @pl.when(d > 0)
            def _():
                remote(obuf.at[peer, rows], res.at[col, rows],
                       o_send.at[d - 1], o_recv.at[d - 1], {'col': peer}).start()

    up, down = near
    for e in range(hh):
        third(e, 0).start()
    send_part(2)
    take_rows(0)
    complete(0)
    send_part(3)
    run(-1, do_ex=False)
    take_rows(1)
    run(0)

    def body(t, carry):
        @pl.when(t == 1)
        def _():
            for e in range(hh):
                whole_second(e, near[e]).wait_recv()
                beyond(e).start()
            for e in range(hh):
                third(e, near[e]).start()
                arrived(e, near[1 - e])
            take_rows(2)

        @pl.when(t == 2)
        def _():
            complete(up)

        @pl.when(t == 3)
        def _():
            complete(down)

        @pl.when(t == 4)
        def _():
            for e in range(hh):
                arrived(e, 2)

        @pl.when(t == 6)
        def _():
            take_rows(3)

        @pl.when(t == 7)
        def _():
            complete(2)

        make(t - 1)
        run(t)
        give(t - 1)
        return carry

    lax.fori_loop(1, n_step, body, 0)
    make(n_step - 1)
    give(n_step - 1)

    mine = pltpu.make_async_copy(obuf.at[col], res.at[col], own_sem)
    mine.start()
    for e in range(hh):
        for d in range(1, n_col):
            first(e, d).wait_send()
        for d in near:
            whole_second(e, d).wait_send()
        beyond(e).wait_send()
        for d in range(n_row):
            third(e, d).wait_send()
    for q in range(n_part):
        for d in range(1, n_col):
            rows_out(q, d).wait_send()
    for d in range(1, n_col):
        peer = at_col(d)
        whole = remote(obuf.at[peer], res.at[col], o_send.at[d - 1], o_recv.at[d - 1], {'col': peer})
        whole.wait_send()
        whole.wait_recv()
    mine.wait()


def solution(mesh):
    n_col = mesh.shape['col']
    n_row = mesh.shape['row']
    tile_spec = P(('dp', 'row'), 'col', None)
    hbm = pl.BlockSpec(memory_space=pltpu.HBM)
    n_part = 4

    def per_device(pair_tile, res_mask, ln_gamma, ln_beta, w_q, w_k, w_v, w_b, w_g, w_o):
        row_len, col_len, chan = pair_tile.shape
        heads = w_b.shape[1]
        hd = chan // heads
        n = res_mask.shape[0]
        own = row_len // n_col
        hc = chan // 2
        lanes = 2 * col_len
        dma = pltpu.SemaphoreType.DMA
        res = pl.pallas_call(
            functools.partial(attn_kernel, n_col, n_row),
            in_specs=[hbm] * 10,
            out_specs=hbm,
            out_shape=jax.ShapeDtypeStruct((n_col, own, hc, lanes), BF16),
            scratch_shapes=[
                pltpu.VMEM((col_len, chan, row_len), BF16),
                pltpu.VMEM((1, n), res_mask.dtype),
                pltpu.VMEM((1, chan), F32),
                pltpu.VMEM((1, chan), F32),
                pltpu.VMEM(w_q.shape, BF16),
                pltpu.VMEM(w_k.shape, BF16),
                pltpu.VMEM(w_v.shape, BF16),
                pltpu.VMEM(w_g.shape, BF16),
                pltpu.VMEM((heads, chan), BF16),
                pltpu.VMEM(w_o.shape, BF16),
                pltpu.VMEM((heads, col_len, row_len), BF16),
                pltpu.VMEM((row_len, hc, lanes), BF16),
                pltpu.VMEM((n_col, own, hc, lanes), BF16),
                pltpu.VMEM((n_row, heads, n, row_len), BF16),
                pltpu.VMEM((n_row, heads // 2, n, 2 * row_len), F32),
                pltpu.VMEM((n, row_len), F32),
                pltpu.VMEM((n_row, own, chan, row_len), F32),
                pltpu.VMEM((n_row, own * heads // 2, chan, 2 * row_len), BF16),
                pltpu.VMEM((own, n, chan), BF16),
                pltpu.VMEM((own * heads // 2, 2 * hd, n), BF16),
                pltpu.VMEM((n_row, own * heads // 2, hd, 2 * row_len), F32),
                pltpu.VMEM((own // n_part * heads // 2, n, 2 * row_len), F32),
                pltpu.VMEM((own // n_part * heads // 2, 1, 2 * row_len), F32),
                pltpu.VMEM((n_row, own * heads // 2, hd, 2 * row_len), BF16),
                pltpu.VMEM((n_col, own, hc, lanes), BF16),
                pltpu.VMEM((4 * chan, chan), BF16),
                pltpu.VMEM((chan, chan), BF16),
                pltpu.VMEM((2, chan, row_len), F32),
                dma((10,)),
                dma((heads // 2, n_col - 1)), dma((heads // 2, n_col - 1)),
                dma((n_part, n_col - 1)), dma((n_part, n_col - 1)),
                dma((heads // 2, n_row - 1)), dma((heads // 2, n_row - 1)),
                dma((heads // 2, n_row)), dma((heads // 2, n_row)),
                dma((n_col - 1,)), dma((n_col - 1,)), dma,
            ],
            compiler_params=pltpu.CompilerParams(
                collective_id=0, has_side_effects=True, vmem_limit_bytes=56 << 20),
            name='attention',
        )(jnp.transpose(pair_tile, (1, 2, 0)), res_mask.reshape(1, n), ln_gamma.reshape(1, chan),
          ln_beta.reshape(1, chan), w_q, w_k, w_v, w_g, w_b.T, w_o)

        pairs = 16
        out = pl.pallas_call(
            unpack_kernel,
            grid=(hc // pairs,),
            in_specs=[pl.BlockSpec((row_len, pairs, lanes), lambda i: (0, i, 0))],
            out_specs=pl.BlockSpec((col_len, 2, pairs, row_len), lambda i: (0, 0, i, 0)),
            out_shape=jax.ShapeDtypeStruct((col_len, 2, hc, row_len), BF16),
            name='unpack',
        )(res.reshape(row_len, hc, lanes)).reshape(col_len, chan, row_len)
        return jnp.transpose(out, (2, 0, 1))

    return jax.shard_map(per_device, mesh=mesh,
                         in_specs=(tile_spec, P('dp'), P(), P(), P(), P(), P(), P(), P(), P()),
                         out_specs=tile_spec, check_vma=False)
```
